32 devices in a mesh: row: 4 (over x, core), col: 4 (over z), depth: 2 (over y).
Axes of the slice: x: 2, y: 2, z: 4, core: 2. Of those that a mesh axis runs over, the one named last changes fastest.
Arguments:
- tokens: bfloat16 [512, 4096], P(('col', 'depth'), 'row'), may hold values from -6 to 6
- w_gate: bfloat16 [4096, 14336], P('row', 'col'), may hold values from -0.09375 to 0.09375
- w_up: bfloat16 [4096, 14336], P('row', 'col'), may hold values from -0.09375 to 0.09375
- w_down: bfloat16 [14336, 4096], P('col', 'row'), may hold values from -0.046875 to 0.046875
- cotangent: bfloat16 [512, 4096], P(('col', 'depth'), 'row'), may hold values from -0.25 to 0.25
Outputs:
- mixed: bfloat16 [512, 4096], P(('col', 'depth'), 'row')
- grad_gate: bfloat16 [4096, 14336], P(('row', 'depth'), 'col')
- grad_up: bfloat16 [4096, 14336], P(('row', 'depth'), 'col')
- grad_down: bfloat16 [14336, 4096], P(('col', 'depth'), 'row')
The draws below stay inside these ranges and needn't reach their ends.
All inputs are finite; a program needn't handle non-finite values.
Results may differ from the reference program's by a relative error of at most 0.025.
Values may be sent and summed in bfloat16 or wider, within the bound.
A program may use at most 128 MiB of HBM per device.

```python
import jax
import jax.numpy as jnp
from jax import lax

D = 4096
FF = 14336
TOK_DEV = 64
TOKENS = 512
N_ROW = 4
N_COL = 4
N_DEPTH = 2


def steps_of(own_key, shape, pieces, low, top_value):
    level, own = 1.0, jax.random.fold_in(own_key, 6)
    for axis_at, parts in pieces:
        draws = jnp.exp(jax.random.uniform(jax.random.fold_in(own, axis_at), (parts,), jnp.float32, low / len(pieces), top_value / len(pieces)))
        level = level * jnp.repeat(draws, shape[axis_at] // parts).reshape([-1 if axis == axis_at else 1 for axis in range(len(shape))])
    return level


def noise(stream_key, shape, width, reach, split=(), kind=jnp.bfloat16):
    gain = steps_of(stream_key, shape, split, -0.22, 0.18) if split else 1.0
    values = jax.random.normal(stream_key, shape, jnp.float32) * width * gain
    return jnp.minimum(jnp.maximum(values, -reach), reach).astype(kind)


def setup_inputs(seed: int = 0) -> dict:
    splits = jax.random.split(jax.random.key(seed), 6)
    tokens = noise(splits[0], (TOKENS, D), 1.0, 6.0, ((0, 8), (1, 4)))
    w_gate = noise(splits[1], (D, FF), D ** -0.5, 0.09375, ((0, 4), (1, 4)))
    w_up = noise(splits[2], (D, FF), D ** -0.5, 0.09375, ((0, 4), (1, 4)))
    w_down = noise(splits[3], (FF, D), FF ** -0.5, 0.046875, ((0, 4), (1, 4)))
    cotangent = noise(splits[4], (TOKENS, D), (TOKENS ** -0.5), 0.25, ((0, 8), (1, 4)))
    return dict(tokens=tokens, w_gate=w_gate, w_up=w_up, w_down=w_down, cotangent=cotangent)


COLS_CONTRACT = (((1,), (1,)), ((), ()))
ROWS_CONTRACT = (((0,), (0,)), ((), ()))


def rounded_add(running, addend):
    rounded = lax.optimization_barrier(addend.astype(jnp.bfloat16))
    return running + rounded.astype(jnp.float32)


def layer_rows(array, layer_index):
    shaped = array.reshape(N_COL, N_DEPTH, TOK_DEV, array.shape[1])
    return shaped[:, layer_index].reshape(N_COL * TOK_DEV, array.shape[1])


def reference(tokens, w_gate, w_up, w_down, cotangent):
    feat_width = D // N_ROW
    token_count = tokens.shape[0]
    gate_sum = jnp.zeros((token_count, FF), jnp.float32)
    up_sum = jnp.zeros((token_count, FF), jnp.float32)
    hidden_grad = jnp.zeros((token_count, FF), jnp.float32)
    for block_index in range(N_ROW):
        lower_edge = block_index * feat_width
        upper_edge = lower_edge + feat_width
        tok_block = tokens[:, lower_edge:upper_edge]
        gate_sum = rounded_add(gate_sum, jnp.dot(tok_block, w_gate[lower_edge:upper_edge], preferred_element_type=jnp.float32))
        up_sum = rounded_add(up_sum, jnp.dot(tok_block, w_up[lower_edge:upper_edge], preferred_element_type=jnp.float32))
        hidden_grad = rounded_add(hidden_grad, lax.dot_general(cotangent[:, lower_edge:upper_edge], w_down[:, lower_edge:upper_edge], COLS_CONTRACT, preferred_element_type=jnp.float32))
    hidden = (jax.nn.silu(gate_sum) * up_sum).astype(jnp.bfloat16)
    mixed = jnp.dot(hidden, w_down, preferred_element_type=jnp.float32).astype(jnp.bfloat16)
    sigmoid_gate = jax.nn.sigmoid(gate_sum)
    d_gate = (hidden_grad * up_sum * sigmoid_gate * (1.0 + gate_sum * (1.0 - sigmoid_gate))).astype(jnp.bfloat16)
    d_up = (hidden_grad * gate_sum * sigmoid_gate).astype(jnp.bfloat16)
    grad_gate = jnp.zeros((D, FF), jnp.float32)
    grad_up = jnp.zeros((D, FF), jnp.float32)
    grad_down = jnp.zeros((FF, D), jnp.float32)
    for layer_index in range(N_DEPTH):
        tok_layer = layer_rows(tokens, layer_index)
        grad_gate = rounded_add(grad_gate, lax.dot_general(tok_layer, layer_rows(d_gate, layer_index), ROWS_CONTRACT, preferred_element_type=jnp.float32))
        grad_up = rounded_add(grad_up, lax.dot_general(tok_layer, layer_rows(d_up, layer_index), ROWS_CONTRACT, preferred_element_type=jnp.float32))
        grad_down = rounded_add(grad_down, lax.dot_general(layer_rows(hidden, layer_index), layer_rows(cotangent, layer_index), ROWS_CONTRACT, preferred_element_type=jnp.float32))
    return (mixed, grad_gate.astype(jnp.bfloat16), grad_up.astype(jnp.bfloat16), grad_down.astype(jnp.bfloat16))
```

```python
import functools

import jax
import jax.numpy as jnp
from jax import lax
from jax.experimental import pallas as pl
from jax.experimental.pallas import tpu as pltpu
from jax.sharding import PartitionSpec as P

COLS_CONTRACT = (((1,), (1,)), ((), ()))
ROWS_CONTRACT = (((0,), (0,)), ((), ()))


def gate_grads(hidden_grad, gate_sum, up_sum):
    sigmoid_gate = jax.nn.sigmoid(gate_sum)
    d_gate = (hidden_grad * up_sum * sigmoid_gate * (1.0 + gate_sum * (1.0 - sigmoid_gate))).astype(
        jnp.bfloat16
    )
    d_up = (hidden_grad * gate_sum * sigmoid_gate).astype(jnp.bfloat16)
    return (d_gate, d_up)


def layered_device(tokens, w_gate, w_up, w_down, cotangent):
    hid_width = w_gate.shape[1]
    token_rows = lax.all_gather(tokens, "col", axis=0, tiled=True)
    row_piece = token_rows
    joined = lax.psum_scatter(
        jnp.concatenate(
            [
                jnp.dot(row_piece, w_gate, preferred_element_type=jnp.float32),
                jnp.dot(row_piece, w_up, preferred_element_type=jnp.float32),
            ],
            axis=1,
        ).astype(jnp.bfloat16),
        "row",
        scatter_dimension=0,
        tiled=True,
    ).astype(jnp.float32)
    gate_sum = joined[:, :hid_width]
    up_sum = joined[:, hid_width:]
    hidden = (jax.nn.silu(gate_sum) * up_sum).astype(jnp.bfloat16)
    hidden_rows = lax.all_gather(hidden, "row", axis=0, tiled=True)
    row_piece = hidden_rows
    mixed = lax.psum_scatter(
        jnp.dot(row_piece, w_down, preferred_element_type=jnp.float32).astype(jnp.bfloat16),
        "col",
        scatter_dimension=0,
        tiled=True,
    )
    cot_rows = lax.all_gather(cotangent, "col", axis=0, tiled=True)
    row_piece = cot_rows
    hidden_grad = lax.psum_scatter(
        lax.dot_general(
            row_piece, w_down, COLS_CONTRACT, preferred_element_type=jnp.float32
        ).astype(jnp.bfloat16),
        "row",
        scatter_dimension=0,
        tiled=True,
    ).astype(jnp.float32)
    d_gate, d_up = gate_grads(hidden_grad, gate_sum, up_sum)
    d_gate_rows, d_up_rows = (
        lax.all_gather(d_gate, "row", axis=0, tiled=True),
        lax.all_gather(d_up, "row", axis=0, tiled=True),
    )
    down_term = lax.dot_general(
        hidden_rows, cot_rows, ROWS_CONTRACT, preferred_element_type=jnp.float32
    )
    grad_down = lax.psum_scatter(
        down_term.astype(jnp.bfloat16), "depth", scatter_dimension=0, tiled=True
    )
    layer_tokens = lax.all_to_all(token_rows, "depth", split_axis=1, concat_axis=0, tiled=True)
    block_rows = token_rows.shape[0]
    empty_grad = jnp.zeros((layer_tokens.shape[1], d_gate_rows.shape[1]), jnp.float32)
    first_row = jnp.int32(0)
    gate_total = empty_grad
    up_total = empty_grad
    gate_piece = lax.all_gather(d_gate_rows, "depth", axis=0, tiled=True)
    up_piece = lax.all_gather(d_up_rows, "depth", axis=0, tiled=True)
    for sub_index in range(gate_piece.shape[0] // block_rows):
        gate_block = gate_piece[sub_index * block_rows : (sub_index + 1) * block_rows]
        up_block = up_piece[sub_index * block_rows : (sub_index + 1) * block_rows]
        offset = first_row + sub_index * block_rows
        tok_block = lax.dynamic_slice_in_dim(layer_tokens, offset, block_rows, 0)
        gate_part = lax.optimization_barrier(
            lax.dot_general(
                tok_block, gate_block, ROWS_CONTRACT, preferred_element_type=jnp.float32
            ).astype(jnp.bfloat16)
        )
        up_part = lax.optimization_barrier(
            lax.dot_general(
                tok_block, up_block, ROWS_CONTRACT, preferred_element_type=jnp.float32
            ).astype(jnp.bfloat16)
        )
        gate_total = gate_total + gate_part.astype(jnp.float32)
        up_total = up_total + up_part.astype(jnp.float32)
    return (mixed, gate_total.astype(jnp.bfloat16), up_total.astype(jnp.bfloat16), grad_down)


MESH = pl.DeviceIdType.MESH
VMEM_LIMIT = 66_000_000


def f32(x):
    return x.astype(jnp.float32)


def bf16(x):
    return x.astype(jnp.bfloat16)


def rows_dot(x, y):
    return lax.dot_general(x, y, ROWS_CONTRACT, preferred_element_type=jnp.float32)


def exchange_kernel(
    n_row,
    n_col,
    tok_in,
    gate_in,
    up_in,
    down_in,
    cot_in,
    mixed_out,
    tok_out,
    cot_out,
    hid_out,
    dgate_out,
    dup_out,
    tok_v,
    cot_v,
    tok_far,
    cot_far,
    gate_v,
    up_v,
    down_v,
    core_send_v,
    core_recv_v,
    own_v,
    x_send_v,
    x_recv_v,
    near_v,
    far_v,
    far_hid_v,
    mix_own_v,
    mix_send_v,
    mix_recv_v,
    load_tok_sem,
    load_w_sem,
    z_send,
    z_recv,
    yt_send,
    yt_recv,
    core_send,
    core_recv,
    x_send,
    x_recv,
    near_send,
    near_recv,
    y_send,
    y_recv,
    yh_send,
    yh_recv,
    fwd_send,
    fwd_recv,
    fwdh_send,
    fwdh_recv,
    mix_send,
    mix_recv,
    out_sem,
):
    row, col, layer = lax.axis_index("row"), lax.axis_index("col"), lax.axis_index("depth")
    core = row % 2
    other = 1 - core
    far_layer = 1 - layer
    blocks, rows, feats = tok_v.shape
    half_feats = tok_far.shape[2]
    quarter = gate_v.shape[2]
    units = x_send_v.shape[0]

    core_id = (row + 1 - 2 * core, col, layer)
    x_id = ((row + 2) % n_row, col, layer)
    y_id = (row, col, far_layer)
    z_ids = {
        1: (row, n_col - 1 - col, layer),
        2: (row, (col + 2) % n_col, layer),
        3: (row, col + 1 - 2 * (col % 2), layer),
    }

    def remote(src, dst, send, recv, device):
        return pltpu.make_async_remote_copy(
            src_ref=src, dst_ref=dst, send_sem=send, recv_sem=recv, device_id=device, device_id_type=MESH
        )

    def load_weight(array, part):
        source = (gate_in, up_in, down_in)[array]
        target = (gate_v, up_v, down_v)[array]
        span = slice(part * quarter, (part + 1) * quarter)
        view = source.at[span, :] if array == 2 else source.at[:, span]
        return pltpu.make_async_copy(view, target.at[part], load_w_sem.at[array, part])

    load_tok = pltpu.make_async_copy(tok_in, tok_v.at[0], load_tok_sem.at[0])
    load_cot = pltpu.make_async_copy(cot_in, cot_v.at[0], load_tok_sem.at[1])
    load_tok.start()
    load_cot.start()
    for pair in range(2):
        for array in range(3):
            for part in (2 * pair, 2 * pair + 1):
                load_weight(array, part).start()

    barrier = pltpu.get_barrier_semaphore()
    peers = [core_id, x_id, y_id] + [z_ids[b] for b in range(1, blocks)]
    for peer in peers:
        pl.semaphore_signal(barrier, inc=1, device_id=peer, device_id_type=MESH)
    pl.semaphore_wait(barrier, len(peers))

    def z_copy(array, b):
        buffer = (tok_v, cot_v)[array]
        return remote(buffer.at[0], buffer.at[b], z_send.at[array, b], z_recv.at[array, b], z_ids[b])

    load_tok.wait()
    for b in range(1, blocks):
        z_copy(0, b).start()
    load_cot.wait()
    for b in range(1, blocks):
        z_copy(1, b).start()

    def yt_copy(b, array):
        if array == 0:
            lanes = pl.ds(pl.multiple_of(far_layer * half_feats, 128), half_feats)
            return remote(tok_v.at[b, :, lanes], tok_far.at[b], yt_send.at[b, 0], yt_recv.at[b, 0], y_id)
        return remote(cot_v.at[b], cot_far.at[b], yt_send.at[b, 1], yt_recv.at[b, 1], y_id)

    def out_rows(b, far):
        return pl.ds(pl.multiple_of((b + far * blocks) * rows, rows), rows)

    def send_out(src, dst, slot):
        pltpu.make_async_copy(src, dst, out_sem.at[slot]).start()

    def core_copy(u, a):
        return remote(
            core_send_v.at[u, a], core_recv_v.at[u, a], core_send.at[u, a], core_recv.at[u, a], core_id
        )

    def x_copy(u, a):
        return remote(x_send_v.at[u, a], x_recv_v.at[u, a], x_send.at[u, a], x_recv.at[u, a], x_id)

    def near_copy(u):
        return remote(near_v.at[core, u], near_v.at[core, u], near_send.at[u], near_recv.at[u], core_id)

    def near_arrival(u):
        return remote(near_v.at[other, u], near_v.at[other, u], near_send.at[u], near_recv.at[u], core_id)

    def y_copy(u):
        return remote(near_v.at[core, u, 0:2], far_v.at[core, u], y_send.at[u], y_recv.at[u], y_id)

    def yh_copy(u, b):
        return remote(near_v.at[core, u, 2], far_hid_v.at[core, b], yh_send.at[b], yh_recv.at[b], y_id)

    def fwd_copy(u):
        return remote(far_v.at[core, u], far_v.at[core, u], fwd_send.at[u], fwd_recv.at[u], core_id)

    def fwd_arrival(u):
        return remote(far_v.at[other, u], far_v.at[other, u], fwd_send.at[u], fwd_recv.at[u], core_id)

    def fwdh_copy(b):
        return remote(far_hid_v.at[core, b], far_hid_v.at[core, b], fwdh_send.at[b], fwdh_recv.at[b], core_id)

    def fwdh_arrival(b):
        return remote(
            far_hid_v.at[other, b], far_hid_v.at[other, b], fwdh_send.at[b], fwdh_recv.at[b], core_id
        )

    def mix_copy(b):
        return remote(mix_send_v.at[b], mix_recv_v.at[b], mix_send.at[b], mix_recv.at[b], z_ids[b])

    def grads_out(pair, u, side, far):
        q, b = u % 2, u // 2
        lanes = pl.ds(pl.multiple_of((2 * q + side) * quarter, 128), quarter)
        send_out(pair[0], dgate_out.at[out_rows(b, far), lanes], 3)
        send_out(pair[1], dup_out.at[out_rows(b, far), lanes], 4)

    def hid_to_out(src, b, side, far):
        lanes = pl.ds(pl.multiple_of(side * quarter, 128), quarter)
        send_out(src, hid_out.at[out_rows(b, far), lanes], 2)

    def products(u, array):
        q, b = u % 2, u // 2
        for side, keep in ((other, False), (core, True)):
            part = 2 * q + side
            if array == 2:
                value = lax.dot_general(
                    cot_v[b], down_v[part], COLS_CONTRACT, preferred_element_type=jnp.float32
                )
            else:
                weight = (gate_v, up_v)[array]
                value = jnp.dot(tok_v[b], weight[part], preferred_element_type=jnp.float32)
            if keep:
                own_v[u, array] = value
            else:
                core_send_v[u, array] = bf16(value)
                core_copy(u, array).start()

    def finish(u, array):
        core_copy(u, array).wait_recv()
        total = own_v[u, array] + f32(core_recv_v[u, array])
        own_v[u, array] = total
        x_send_v[u, array] = bf16(total)
        x_copy(u, array).start()

    def wait_weight(u, array):
        q = u % 2
        for pair in range(2):

            @pl.when((u < 2) & (q == pair))
            def _():
                load_weight(array, 2 * pair).wait()
                load_weight(array, 2 * pair + 1).wait()

    def compute_unit(u):
        q, b = u % 2, u // 2

        for static_b in range(1, blocks):

            @pl.when((b == static_b) & (q == 0))
            def _():
                z_copy(0, static_b).wait_recv()
                z_copy(1, static_b).wait_recv()

        @pl.when(q == 0)
        def _():
            own_lanes = pl.ds(pl.multiple_of(layer * half_feats, 128), half_feats)
            yt_copy(b, 0).start()
            yt_copy(b, 1).start()
            send_out(tok_v.at[b, :, own_lanes], tok_out.at[out_rows(b, 0), :], 0)
            send_out(cot_v.at[b], cot_out.at[out_rows(b, 0), :], 1)

        wait_weight(u, 0)
        products(u, 0)
        wait_weight(u, 1)
        products(u, 1)
        finish(u, 0)
        wait_weight(u, 2)
        products(u, 2)
        finish(u, 1)
        finish(u, 2)

    row_step = 16

    def combine(u):
        q, b = u % 2, u // 2
        for a in range(3):
            x_copy(u, a).wait_recv()

        def some_rows(i, carry):
            span = pl.ds(pl.multiple_of(i * row_step, row_step), row_step)
            gate_sum = own_v[u, 0, span, :] + f32(x_recv_v[u, 0, span, :])
            up_sum = own_v[u, 1, span, :] + f32(x_recv_v[u, 1, span, :])
            hidden_grad = own_v[u, 2, span, :] + f32(x_recv_v[u, 2, span, :])
            sigmoid_gate = jax.nn.sigmoid(gate_sum)
            swish = gate_sum * sigmoid_gate
            near_v[core, u, 2, span, :] = bf16(swish * up_sum)
            near_v[core, u, 1, span, :] = bf16(hidden_grad * swish)
            near_v[core, u, 0, span, :] = bf16(
                hidden_grad * up_sum * sigmoid_gate * (1.0 + gate_sum * (1.0 - sigmoid_gate))
            )
            return carry

        lax.fori_loop(0, rows // row_step, some_rows, 0)
        near_copy(u).start()
        y_copy(u).start()

        @pl.when(q == far_layer)
        def _():
            yh_copy(u, b).start()

        grads_out((near_v.at[core, u, 0], near_v.at[core, u, 1]), u, core, 0)

        @pl.when(q == layer)
        def _():
            hid_to_out(near_v.at[core, u, 2], b, core, 0)

    def near_arrived(u):
        q, b = u % 2, u // 2
        near_arrival(u).wait_recv()
        grads_out((near_v.at[other, u, 0], near_v.at[other, u, 1]), u, other, 0)

        @pl.when(q == layer)
        def _():
            hid_to_out(near_v.at[other, u, 2], b, other, 0)

        @pl.when(q == 1)
        def _():
            total = jnp.zeros((rows, feats), jnp.float32)
            for half in range(2):
                for side in range(2):
                    total = total + jnp.dot(
                        near_v[side, 2 * b + half, 2],
                        down_v[2 * half + side],
                        preferred_element_type=jnp.float32,
                    )

            @pl.when(b == 0)
            def _():
                mix_own_v[...] = total

            @pl.when(b > 0)
            def _():
                mix_send_v[b] = bf16(total)

            for static_b in range(1, blocks):

                @pl.when(b == static_b)
                def _():
                    mix_copy(static_b).start()

    def far_arrived(u):
        q, b = u % 2, u // 2
        y_copy(u).wait_recv()
        fwd_copy(u).start()
        grads_out((far_v.at[core, u, 0], far_v.at[core, u, 1]), u, core, 1)

        @pl.when(q == layer)
        def _():
            yh_copy(u, b).wait_recv()
            fwdh_copy(b).start()
            hid_to_out(far_hid_v.at[core, b], b, core, 1)

        @pl.when(q == 0)
        def _():
            yt_copy(b, 0).wait_recv()
            yt_copy(b, 1).wait_recv()
            send_out(tok_far.at[b], tok_out.at[out_rows(b, 1), :], 0)
            send_out(cot_far.at[b], cot_out.at[out_rows(b, 1), :], 1)

    def forwarded(u):
        q, b = u % 2, u // 2
        fwd_arrival(u).wait_recv()
        grads_out((far_v.at[other, u, 0], far_v.at[other, u, 1]), u, other, 1)

        @pl.when(q == layer)
        def _():
            fwdh_arrival(b).wait_recv()
            hid_to_out(far_hid_v.at[other, b], b, other, 1)

    stages = ((compute_unit, 0), (combine, 2), (near_arrived, 3), (far_arrived, 4), (forwarded, 5))

    def step(s, carry):
        for stage, lag in stages:

            @pl.when((s >= lag) & (s < units + lag))
            def _():
                stage(s - lag)

        return carry

    lax.fori_loop(0, units + stages[-1][1], step, 0)

    total = mix_own_v[...]
    for b in range(1, blocks):
        mix_copy(b).wait_recv()
        total = total + f32(mix_recv_v[b])
    mixed_out[...] = bf16(total)

    for b in range(1, blocks):
        z_copy(0, b).wait_send()
        z_copy(1, b).wait_send()
        mix_copy(b).wait_send()

    def drain_block(b, carry):
        yt_copy(b, 0).wait_send()
        yt_copy(b, 1).wait_send()
        yh_copy(2 * b, b).wait_send()
        fwdh_copy(b).wait_send()
        return carry

    def drain_unit(u, carry):
        for a in range(3):
            core_copy(u, a).wait_send()
            x_copy(u, a).wait_send()
        near_copy(u).wait_send()
        y_copy(u).wait_send()
        fwd_copy(u).wait_send()
        return carry

    lax.fori_loop(0, blocks, drain_block, 0)
    lax.fori_loop(0, units, drain_unit, 0)
    for slot, out in enumerate((tok_out, cot_out, hid_out, dgate_out, dup_out)):
        pltpu.make_async_copy(out, out, out_sem.at[slot]).wait()


def grid_device(n_row, n_col, tokens, w_gate, w_up, w_down, cotangent):
    rows, feats = tokens.shape
    hid = w_gate.shape[1]
    quarter = hid // 4
    blocks = n_col
    units = 2 * blocks
    all_rows = 2 * blocks * rows
    narrow, wide = jnp.bfloat16, jnp.float32
    dma = pltpu.SemaphoreType.DMA
    scratch = [
        pltpu.VMEM((blocks, rows, feats), narrow),
        pltpu.VMEM((blocks, rows, feats), narrow),
        pltpu.VMEM((blocks, rows, feats // 2), narrow),
        pltpu.VMEM((blocks, rows, feats), narrow),
        pltpu.VMEM((4, feats, quarter), narrow),
        pltpu.VMEM((4, feats, quarter), narrow),
        pltpu.VMEM((4, quarter, feats), narrow),
        pltpu.VMEM((units, 3, rows, quarter), narrow),
        pltpu.VMEM((units, 3, rows, quarter), narrow),
        pltpu.VMEM((units, 3, rows, quarter), wide),
        pltpu.VMEM((units, 3, rows, quarter), narrow),
        pltpu.VMEM((units, 3, rows, quarter), narrow),
        pltpu.VMEM((2, units, 3, rows, quarter), narrow),
        pltpu.VMEM((2, units, 2, rows, quarter), narrow),
        pltpu.VMEM((2, blocks, rows, quarter), narrow),
        pltpu.VMEM((rows, feats), wide),
        pltpu.VMEM((blocks, rows, feats), narrow),
        pltpu.VMEM((blocks, rows, feats), narrow),
        dma((2,)),
        dma((3, 4)),
        dma((2, blocks)),
        dma((2, blocks)),
        dma((blocks, 2)),
        dma((blocks, 2)),
        dma((units, 3)),
        dma((units, 3)),
        dma((units, 3)),
        dma((units, 3)),
        dma((units,)),
        dma((units,)),
        dma((units,)),
        dma((units,)),
        dma((blocks,)),
        dma((blocks,)),
        dma((units,)),
        dma((units,)),
        dma((blocks,)),
        dma((blocks,)),
        dma((blocks,)),
        dma((blocks,)),
        dma((5,)),
    ]
    mixed, tok, cot, hidden, d_gate, d_up = pl.pallas_call(
        functools.partial(exchange_kernel, n_row, n_col),
        out_shape=[
            jax.ShapeDtypeStruct((rows, feats), narrow),
            jax.ShapeDtypeStruct((all_rows, feats // 2), narrow),
            jax.ShapeDtypeStruct((all_rows, feats), narrow),
            jax.ShapeDtypeStruct((all_rows, hid // 2), narrow),
            jax.ShapeDtypeStruct((all_rows, hid), narrow),
            jax.ShapeDtypeStruct((all_rows, hid), narrow),
        ],
        in_specs=[pl.BlockSpec(memory_space=pl.ANY)] * 5,
        out_specs=[pl.BlockSpec(memory_space=pltpu.VMEM)] + [pl.BlockSpec(memory_space=pl.ANY)] * 5,
        scratch_shapes=scratch,
        compiler_params=pltpu.CompilerParams(
            collective_id=0, has_side_effects=True, vmem_limit_bytes=VMEM_LIMIT
        ),
    )(tokens, w_gate, w_up, w_down, cotangent)
    grad_gate = bf16(rows_dot(tok, d_gate))
    grad_up = bf16(rows_dot(tok, d_up))
    grad_down = bf16(rows_dot(hidden, cot))
    return (mixed, grad_gate, grad_up, grad_down)


def solution(mesh):
    placed = (
        P(("col", "depth"), "row"),
        P("row", "col"),
        P("row", "col"),
        P("col", "row"),
        P(("col", "depth"), "row"),
    )
    n_row, n_col = mesh.shape["row"], mesh.shape["col"]
    if (n_row, n_col, mesh.shape["depth"]) == (4, 4, 2):
        per_device = functools.partial(grid_device, n_row, n_col)
    else:
        per_device = layered_device
    return jax.shard_map(
        per_device,
        mesh=mesh,
        in_specs=placed,
        out_specs=(
            P(("col", "depth"), "row"),
            P(("row", "depth"), "col"),
            P(("row", "depth"), "col"),
            P(("col", "depth"), "row"),
        ),
        check_vma=False,
    )
```

```python
import functools

import jax
import jax.numpy as jnp
from jax import lax
from jax.experimental import pallas as pl
from jax.experimental.pallas import tpu as pltpu
from jax.sharding import PartitionSpec as P

COLS_CONTRACT = (((1,), (1,)), ((), ()))
ROWS_CONTRACT = (((0,), (0,)), ((), ()))


def gate_grads(hidden_grad, gate_sum, up_sum):
    sigmoid_gate = jax.nn.sigmoid(gate_sum)
    d_gate = (hidden_grad * up_sum * sigmoid_gate * (1.0 + gate_sum * (1.0 - sigmoid_gate))).astype(
        jnp.bfloat16
    )
    d_up = (hidden_grad * gate_sum * sigmoid_gate).astype(jnp.bfloat16)
    return (d_gate, d_up)


def layered_device(tokens, w_gate, w_up, w_down, cotangent):
    hid_width = w_gate.shape[1]
    token_rows = lax.all_gather(tokens, "col", axis=0, tiled=True)
    row_piece = token_rows
    joined = lax.psum_scatter(
        jnp.concatenate(
            [
                jnp.dot(row_piece, w_gate, preferred_element_type=jnp.float32),
                jnp.dot(row_piece, w_up, preferred_element_type=jnp.float32),
            ],
            axis=1,
        ).astype(jnp.bfloat16),
        "row",
        scatter_dimension=0,
        tiled=True,
    ).astype(jnp.float32)
    gate_sum = joined[:, :hid_width]
    up_sum = joined[:, hid_width:]
    hidden = (jax.nn.silu(gate_sum) * up_sum).astype(jnp.bfloat16)
    hidden_rows = lax.all_gather(hidden, "row", axis=0, tiled=True)
    row_piece = hidden_rows
    mixed = lax.psum_scatter(
        jnp.dot(row_piece, w_down, preferred_element_type=jnp.float32).astype(jnp.bfloat16),
        "col",
        scatter_dimension=0,
        tiled=True,
    )
    cot_rows = lax.all_gather(cotangent, "col", axis=0, tiled=True)
    row_piece = cot_rows
    hidden_grad = lax.psum_scatter(
        lax.dot_general(
            row_piece, w_down, COLS_CONTRACT, preferred_element_type=jnp.float32
        ).astype(jnp.bfloat16),
        "row",
        scatter_dimension=0,
        tiled=True,
    ).astype(jnp.float32)
    d_gate, d_up = gate_grads(hidden_grad, gate_sum, up_sum)
    d_gate_rows, d_up_rows = (
        lax.all_gather(d_gate, "row", axis=0, tiled=True),
        lax.all_gather(d_up, "row", axis=0, tiled=True),
    )
    down_term = lax.dot_general(
        hidden_rows, cot_rows, ROWS_CONTRACT, preferred_element_type=jnp.float32
    )
    grad_down = lax.psum_scatter(
        down_term.astype(jnp.bfloat16), "depth", scatter_dimension=0, tiled=True
    )
    layer_tokens = lax.all_to_all(token_rows, "depth", split_axis=1, concat_axis=0, tiled=True)
    block_rows = token_rows.shape[0]
    empty_grad = jnp.zeros((layer_tokens.shape[1], d_gate_rows.shape[1]), jnp.float32)
    first_row = jnp.int32(0)
    gate_total = empty_grad
    up_total = empty_grad
    gate_piece = lax.all_gather(d_gate_rows, "depth", axis=0, tiled=True)
    up_piece = lax.all_gather(d_up_rows, "depth", axis=0, tiled=True)
    for sub_index in range(gate_piece.shape[0] // block_rows):
        gate_block = gate_piece[sub_index * block_rows : (sub_index + 1) * block_rows]
        up_block = up_piece[sub_index * block_rows : (sub_index + 1) * block_rows]
        offset = first_row + sub_index * block_rows
        tok_block = lax.dynamic_slice_in_dim(layer_tokens, offset, block_rows, 0)
        gate_part = lax.optimization_barrier(
            lax.dot_general(
                tok_block, gate_block, ROWS_CONTRACT, preferred_element_type=jnp.float32
            ).astype(jnp.bfloat16)
        )
        up_part = lax.optimization_barrier(
            lax.dot_general(
                tok_block, up_block, ROWS_CONTRACT, preferred_element_type=jnp.float32
            ).astype(jnp.bfloat16)
        )
        gate_total = gate_total + gate_part.astype(jnp.float32)
        up_total = up_total + up_part.astype(jnp.float32)
    return (mixed, gate_total.astype(jnp.bfloat16), up_total.astype(jnp.bfloat16), grad_down)


MESH = pl.DeviceIdType.MESH
VMEM_LIMIT = 66_000_000


def f32(x):
    return x.astype(jnp.float32)


def bf16(x):
    return x.astype(jnp.bfloat16)


def rows_dot(x, y):
    return lax.dot_general(x, y, ROWS_CONTRACT, preferred_element_type=jnp.float32)


def exchange_kernel(
    n_row,
    n_col,
    tok_in,
    gate_in,
    up_in,
    down_in,
    cot_in,
    mixed_out,
    tok_out,
    cot_out,
    hid_out,
    dgate_out,
    dup_out,
    tok_v,
    cot_v,
    tok_far,
    cot_far,
    gate_v,
    up_v,
    down_v,
    core_send_v,
    core_recv_v,
    own_v,
    x_send_v,
    x_recv_v,
    near_v,
    far_v,
    far_hid_v,
    mix_own_v,
    mix_acc_v,
    mix_send_v,
    mix_recv_v,
    load_tok_sem,
    load_w_sem,
    z_send,
    z_recv,
    yt_send,
    yt_recv,
    zf_send,
    zf_recv,
    core_send,
    core_recv,
    x_send,
    x_recv,
    near_send,
    near_recv,
    nearh_send,
    nearh_recv,
    y_send,
    y_recv,
    yh_send,
    yh_recv,
    fwd_send,
    fwd_recv,
    fwdh_send,
    fwdh_recv,
    mix_send,
    mix_recv,
    out_sem,
):
    row, col, layer = lax.axis_index("row"), lax.axis_index("col"), lax.axis_index("depth")
    core = row % 2
    other = 1 - core
    far_layer = 1 - layer
    blocks, rows, feats = tok_v.shape
    half_feats = tok_far.shape[2]
    quarter = gate_v.shape[2]
    units = x_send_v.shape[0]

    core_id = (row + 1 - 2 * core, col, layer)
    x_id = ((row + 2) % n_row, col, layer)
    y_id = (row, col, far_layer)
    z_ids = {
        1: (row, n_col - 1 - col, layer),
        2: (row, (col + 2) % n_col, layer),
        3: (row, col + 1 - 2 * (col % 2), layer),
    }

    def remote(src, dst, send, recv, device):
        return pltpu.make_async_remote_copy(
            src_ref=src, dst_ref=dst, send_sem=send, recv_sem=recv, device_id=device, device_id_type=MESH
        )

    def load_weight(array, part):
        source = (gate_in, up_in, down_in)[array]
        target = (gate_v, up_v, down_v)[array]
        span = slice(part * quarter, (part + 1) * quarter)
        view = source.at[span, :] if array == 2 else source.at[:, span]
        return pltpu.make_async_copy(view, target.at[part], load_w_sem.at[array, part])

    load_tok = pltpu.make_async_copy(tok_in, tok_v.at[0], load_tok_sem.at[0])
    load_cot = pltpu.make_async_copy(cot_in, cot_v.at[0], load_tok_sem.at[1])
    load_tok.start()
    load_cot.start()
    def start_weights(pairs):
        for array, pair in pairs:
            for part in (2 * pair, 2 * pair + 1):
                load_weight(array, part).start()

    start_weights([(0, 0)])

    barrier = pltpu.get_barrier_semaphore()
    peers = [core_id, x_id, y_id] + [z_ids[b] for b in range(1, blocks)]
    for peer in peers:
        pl.semaphore_signal(barrier, inc=1, device_id=peer, device_id_type=MESH)
    pl.semaphore_wait(barrier, len(peers))

    def z_copy(array, b):
        buffer = (tok_v, cot_v)[array]
        return remote(buffer.at[0], buffer.at[b], z_send.at[array, b], z_recv.at[array, b], z_ids[b])

    load_tok.wait()
    z_copy(0, 1).start()
    load_cot.wait()
    z_copy(1, 1).start()
    for b in range(2, blocks):
        z_copy(0, b).start()
        z_copy(1, b).start()

    def yt_copy(array):
        if array == 0:
            lanes = pl.ds(pl.multiple_of(far_layer * half_feats, 128), half_feats)
            return remote(tok_v.at[0, :, lanes], tok_far.at[0], yt_send.at[0], yt_recv.at[0], y_id)
        return remote(cot_v.at[0], cot_far.at[0], yt_send.at[1], yt_recv.at[1], y_id)

    yt_copy(0).start()
    yt_copy(1).start()

    def zf_copy(array, b):
        buffer = (tok_far, cot_far)[array]
        return remote(buffer.at[0], buffer.at[b], zf_send.at[array, b], zf_recv.at[array, b], z_ids[b])

    def out_rows(b, far):
        return pl.ds(pl.multiple_of((b + far * blocks) * rows, rows), rows)

    def send_out(src, dst, slot):
        pltpu.make_async_copy(src, dst, out_sem.at[slot]).start()

    def core_copy(u, a):
        return remote(
            core_send_v.at[u, a], core_recv_v.at[u, a], core_send.at[u, a], core_recv.at[u, a], core_id
        )

    def x_copy(u, a):
        return remote(x_send_v.at[u, a], x_recv_v.at[u, a], x_send.at[u, a], x_recv.at[u, a], x_id)

    def near_copy(u, side):
        ref = near_v.at[side, u, 0:2]
        return remote(ref, ref, near_send.at[u], near_recv.at[u], core_id)

    def nearh_copy(u, side):
        ref = near_v.at[side, u, 2]
        return remote(ref, ref, nearh_send.at[u], nearh_recv.at[u], core_id)

    def y_copy(u):
        return remote(near_v.at[core, u, 0:2], far_v.at[core, u], y_send.at[u], y_recv.at[u], y_id)

    def yh_copy(u, b):
        return remote(near_v.at[core, u, 2], far_hid_v.at[core, b], yh_send.at[b], yh_recv.at[b], y_id)

    def fwd_copy(u):
        return remote(far_v.at[core, u], far_v.at[core, u], fwd_send.at[u], fwd_recv.at[u], core_id)

    def fwd_arrival(u):
        return remote(far_v.at[other, u], far_v.at[other, u], fwd_send.at[u], fwd_recv.at[u], core_id)

    def fwdh_copy(b):
        return remote(far_hid_v.at[core, b], far_hid_v.at[core, b], fwdh_send.at[b], fwdh_recv.at[b], core_id)

    def fwdh_arrival(b):
        return remote(
            far_hid_v.at[other, b], far_hid_v.at[other, b], fwdh_send.at[b], fwdh_recv.at[b], core_id
        )

    def mix_copy(b):
        return remote(mix_send_v.at[b], mix_recv_v.at[b], mix_send.at[b], mix_recv.at[b], z_ids[b])

    def grads_out(pair, u, side, far):
        q, b = u % 2, u // 2
        lanes = pl.ds(pl.multiple_of((2 * q + side) * quarter, 128), quarter)
        send_out(pair[0], dgate_out.at[out_rows(b, far), lanes], 3)
        send_out(pair[1], dup_out.at[out_rows(b, far), lanes], 4)

    def hid_to_out(src, b, side, far):
        lanes = pl.ds(pl.multiple_of(side * quarter, 128), quarter)
        send_out(src, hid_out.at[out_rows(b, far), lanes], 2)

    def products(u, array):
        q, b = u % 2, u // 2
        for side, keep in ((other, False), (core, True)):
            part = 2 * q + side
            if array == 2:
                value = lax.dot_general(
                    cot_v[b], down_v[part], COLS_CONTRACT, preferred_element_type=jnp.float32
                )
            else:
                weight = (gate_v, up_v)[array]
                value = jnp.dot(tok_v[b], weight[part], preferred_element_type=jnp.float32)
            if keep:
                own_v[u, array] = value
            else:
                core_send_v[u, array] = bf16(value)
                core_copy(u, array).start()

    def finish(u, array):
        core_copy(u, array).wait_recv()
        total = own_v[u, array] + f32(core_recv_v[u, array])
        own_v[u, array] = total
        x_send_v[u, array] = bf16(total)
        x_copy(u, array).start()

    def wait_weight(u, array):
        q = u % 2
        for pair in range(2):

            @pl.when((u < 2) & (q == pair))
            def _():
                load_weight(array, 2 * pair).wait()
                load_weight(array, 2 * pair + 1).wait()

    def compute_unit(u):
        q, b = u % 2, u // 2

        for static_b in range(1, blocks):

            @pl.when((b == static_b) & (q == 0))
            def _():
                z_copy(0, static_b).wait_recv()

        @pl.when(q == 0)
        def _():
            own_lanes = pl.ds(pl.multiple_of(layer * half_feats, 128), half_feats)
            send_out(tok_v.at[b, :, own_lanes], tok_out.at[out_rows(b, 0), :], 0)

        wait_weight(u, 0)

        @pl.when(u == 0)
        def _():
            start_weights([(1, 0), (2, 0)])

        products(u, 0)
        wait_weight(u, 1)

        @pl.when(u == 0)
        def _():
            start_weights([(0, 1), (1, 1), (2, 1)])

        products(u, 1)
        finish(u, 0)

        for static_b in range(1, blocks):

            @pl.when((b == static_b) & (q == 0))
            def _():
                z_copy(1, static_b).wait_recv()

        @pl.when(q == 0)
        def _():
            send_out(cot_v.at[b], cot_out.at[out_rows(b, 0), :], 1)

        wait_weight(u, 2)
        products(u, 2)
        finish(u, 1)
        finish(u, 2)

    row_step = 16

    def over_rows(body):
        def some_rows(i, carry):
            body(pl.ds(pl.multiple_of(i * row_step, row_step), row_step))
            return carry

        lax.fori_loop(0, rows // row_step, some_rows, 0)

    def activate(u):
        q, b = u % 2, u // 2
        x_copy(u, 0).wait_recv()
        x_copy(u, 1).wait_recv()

        def body(span):
            gate_sum = own_v[u, 0, span, :] + f32(x_recv_v[u, 0, span, :])
            up_sum = own_v[u, 1, span, :] + f32(x_recv_v[u, 1, span, :])
            sigmoid_gate = jax.nn.sigmoid(gate_sum)
            swish = gate_sum * sigmoid_gate
            near_v[core, u, 2, span, :] = bf16(swish * up_sum)
            own_v[u, 0, span, :] = up_sum * sigmoid_gate * (1.0 + gate_sum * (1.0 - sigmoid_gate))
            own_v[u, 1, span, :] = swish

        over_rows(body)
        nearh_copy(u, core).start()

        @pl.when(q == far_layer)
        def _():
            yh_copy(u, b).start()

        @pl.when(q == layer)
        def _():
            hid_to_out(near_v.at[core, u, 2], b, core, 0)

    def mix_part(u):
        q, b = u % 2, u // 2
        nearh_copy(u, other).wait_recv()

        @pl.when(q == layer)
        def _():
            hid_to_out(near_v.at[other, u, 2], b, other, 0)

        part = jnp.zeros((rows, feats), jnp.float32)
        for side in range(2):
            part = part + jnp.dot(
                near_v[side, u, 2], down_v[2 * q + side], preferred_element_type=jnp.float32
            )

        @pl.when(q == 0)
        def _():
            mix_acc_v[...] = part

        @pl.when(u == 1)
        def _():
            mix_own_v[...] = mix_acc_v[...] + part

        @pl.when((q == 1) & (b > 0))
        def _():
            mix_send_v[b] = bf16(mix_acc_v[...] + part)

        for static_b in range(1, blocks):

            @pl.when((q == 1) & (b == static_b))
            def _():
                mix_copy(static_b).start()

    def factors(u):
        x_copy(u, 2).wait_recv()

        def body(span):
            hidden_grad = own_v[u, 2, span, :] + f32(x_recv_v[u, 2, span, :])
            near_v[core, u, 0, span, :] = bf16(hidden_grad * own_v[u, 0, span, :])
            near_v[core, u, 1, span, :] = bf16(hidden_grad * own_v[u, 1, span, :])

        over_rows(body)
        near_copy(u, core).start()
        y_copy(u).start()
        grads_out((near_v.at[core, u, 0], near_v.at[core, u, 1]), u, core, 0)

    def near_arrived(u):
        near_copy(u, other).wait_recv()
        grads_out((near_v.at[other, u, 0], near_v.at[other, u, 1]), u, other, 0)

        @pl.when(u == 1)
        def _():
            yt_copy(0).wait_recv()
            yt_copy(1).wait_recv()
            for b in range(1, blocks):
                zf_copy(0, b).start()
                zf_copy(1, b).start()
            send_out(tok_far.at[0], tok_out.at[out_rows(0, 1), :], 0)
            send_out(cot_far.at[0], cot_out.at[out_rows(0, 1), :], 1)

    def far_arrived(u):
        q, b = u % 2, u // 2
        y_copy(u).wait_recv()
        fwd_copy(u).start()
        grads_out((far_v.at[core, u, 0], far_v.at[core, u, 1]), u, core, 1)

        @pl.when(q == layer)
        def _():
            yh_copy(u, b).wait_recv()
            fwdh_copy(b).start()
            hid_to_out(far_hid_v.at[core, b], b, core, 1)

    def forwarded(u):
        q, b = u % 2, u // 2
        fwd_arrival(u).wait_recv()
        grads_out((far_v.at[other, u, 0], far_v.at[other, u, 1]), u, other, 1)

        @pl.when(q == layer)
        def _():
            fwdh_arrival(b).wait_recv()
            hid_to_out(far_hid_v.at[other, b], b, other, 1)

    stages = (
        (activate, 2),
        (compute_unit, 0),
        (mix_part, 2),
        (factors, 2),
        (near_arrived, 3),
        (far_arrived, 4),
        (forwarded, 5),
    )

    def step(s, carry):
        for stage, lag in stages:

            @pl.when((s >= lag) & (s < units + lag))
            def _():
                stage(s - lag)

        return carry

    lax.fori_loop(0, units + stages[-1][1], step, 0)

    total = mix_own_v[...]
    for b in range(1, blocks):
        mix_copy(b).wait_recv()
        total = total + f32(mix_recv_v[b])
    mixed_out[...] = bf16(total)

    for b in range(1, blocks):
        zf_copy(0, b).wait_recv()
        zf_copy(1, b).wait_recv()
        send_out(tok_far.at[b], tok_out.at[out_rows(b, 1), :], 0)
        send_out(cot_far.at[b], cot_out.at[out_rows(b, 1), :], 1)

    for array in range(2):
        yt_copy(array).wait_send()
        for b in range(1, blocks):
            z_copy(array, b).wait_send()
            zf_copy(array, b).wait_send()
    for b in range(1, blocks):
        mix_copy(b).wait_send()

    def drain_block(b, carry):
        yh_copy(2 * b, b).wait_send()
        fwdh_copy(b).wait_send()
        return carry

    def drain_unit(u, carry):
        for a in range(3):
            core_copy(u, a).wait_send()
            x_copy(u, a).wait_send()
        near_copy(u, core).wait_send()
        nearh_copy(u, core).wait_send()
        y_copy(u).wait_send()
        fwd_copy(u).wait_send()
        return carry

    lax.fori_loop(0, blocks, drain_block, 0)
    lax.fori_loop(0, units, drain_unit, 0)
    for slot, out in enumerate((tok_out, cot_out, hid_out, dgate_out, dup_out)):
        pltpu.make_async_copy(out, out, out_sem.at[slot]).wait()


def gradient_kernel(tok, cot, hidden, d_gate, d_up, grad_gate, grad_up, grad_down, tok_turned):
    @pl.when(pl.program_id(0) == 0)
    def _():
        tok_turned[...] = tok[...].T

    turned = tok_turned[...]
    grad_gate[...] = bf16(jnp.dot(turned, d_gate[...], preferred_element_type=jnp.float32))
    grad_up[...] = bf16(jnp.dot(turned, d_up[...], preferred_element_type=jnp.float32))
    grad_down[...] = bf16(rows_dot(hidden[...], cot[...]))


def gradients(tok, cot, hidden, d_gate, d_up):
    all_rows, half_feats = tok.shape
    feats, half_hid, hid = cot.shape[1], hidden.shape[1], d_gate.shape[1]
    steps = max(n for n in range(1, 8) if half_hid % (128 * n) == 0)
    wide, thin = hid // steps, half_hid // steps
    narrow = jnp.bfloat16
    return pl.pallas_call(
        gradient_kernel,
        grid=(steps,),
        out_shape=[
            jax.ShapeDtypeStruct((half_feats, hid), narrow),
            jax.ShapeDtypeStruct((half_feats, hid), narrow),
            jax.ShapeDtypeStruct((half_hid, feats), narrow),
        ],
        in_specs=[
            pl.BlockSpec((all_rows, half_feats), lambda i: (0, 0)),
            pl.BlockSpec((all_rows, feats), lambda i: (0, 0)),
            pl.BlockSpec((all_rows, thin), lambda i: (0, i)),
            pl.BlockSpec((all_rows, wide), lambda i: (0, i)),
            pl.BlockSpec((all_rows, wide), lambda i: (0, i)),
        ],
        out_specs=[
            pl.BlockSpec((half_feats, wide), lambda i: (0, i)),
            pl.BlockSpec((half_feats, wide), lambda i: (0, i)),
            pl.BlockSpec((thin, feats), lambda i: (i, 0)),
        ],
        scratch_shapes=[pltpu.VMEM((half_feats, all_rows), narrow)],
    )(tok, cot, hidden, d_gate, d_up)


def grid_device(n_row, n_col, tokens, w_gate, w_up, w_down, cotangent):
    rows, feats = tokens.shape
    hid = w_gate.shape[1]
    quarter = hid // 4
    blocks = n_col
    units = 2 * blocks
    all_rows = 2 * blocks * rows
    narrow, wide = jnp.bfloat16, jnp.float32
    dma = pltpu.SemaphoreType.DMA
    scratch = [
        pltpu.VMEM((blocks, rows, feats), narrow),
        pltpu.VMEM((blocks, rows, feats), narrow),
        pltpu.VMEM((blocks, rows, feats // 2), narrow),
        pltpu.VMEM((blocks, rows, feats), narrow),
        pltpu.VMEM((4, feats, quarter), narrow),
        pltpu.VMEM((4, feats, quarter), narrow),
        pltpu.VMEM((4, quarter, feats), narrow),
        pltpu.VMEM((units, 3, rows, quarter), narrow),
        pltpu.VMEM((units, 3, rows, quarter), narrow),
        pltpu.VMEM((units, 3, rows, quarter), wide),
        pltpu.VMEM((units, 3, rows, quarter), narrow),
        pltpu.VMEM((units, 3, rows, quarter), narrow),
        pltpu.VMEM((2, units, 3, rows, quarter), narrow),
        pltpu.VMEM((2, units, 2, rows, quarter), narrow),
        pltpu.VMEM((2, blocks, rows, quarter), narrow),
        pltpu.VMEM((rows, feats), wide),
        pltpu.VMEM((rows, feats), wide),
        pltpu.VMEM((blocks, rows, feats), narrow),
        pltpu.VMEM((blocks, rows, feats), narrow),
        dma((2,)),
        dma((3, 4)),
        dma((2, blocks)),
        dma((2, blocks)),
        dma((2,)),
        dma((2,)),
        dma((2, blocks)),
        dma((2, blocks)),
        dma((units, 3)),
        dma((units, 3)),
        dma((units, 3)),
        dma((units, 3)),
        dma((units,)),
        dma((units,)),
        dma((units,)),
        dma((units,)),
        dma((units,)),
        dma((units,)),
        dma((blocks,)),
        dma((blocks,)),
        dma((units,)),
        dma((units,)),
        dma((blocks,)),
        dma((blocks,)),
        dma((blocks,)),
        dma((blocks,)),
        dma((5,)),
    ]
    mixed, tok, cot, hidden, d_gate, d_up = pl.pallas_call(
        functools.partial(exchange_kernel, n_row, n_col),
        out_shape=[
            jax.ShapeDtypeStruct((rows, feats), narrow),
            jax.ShapeDtypeStruct((all_rows, feats // 2), narrow),
            jax.ShapeDtypeStruct((all_rows, feats), narrow),
            jax.ShapeDtypeStruct((all_rows, hid // 2), narrow),
            jax.ShapeDtypeStruct((all_rows, hid), narrow),
            jax.ShapeDtypeStruct((all_rows, hid), narrow),
        ],
        in_specs=[pl.BlockSpec(memory_space=pl.ANY)] * 5,
        out_specs=[pl.BlockSpec(memory_space=pltpu.VMEM)] + [pl.BlockSpec(memory_space=pl.ANY)] * 5,
        scratch_shapes=scratch,
        compiler_params=pltpu.CompilerParams(
            collective_id=0, has_side_effects=True, vmem_limit_bytes=VMEM_LIMIT
        ),
    )(tokens, w_gate, w_up, w_down, cotangent)
    grad_gate, grad_up, grad_down = gradients(tok, cot, hidden, d_gate, d_up)
    return (mixed, grad_gate, grad_up, grad_down)


def solution(mesh):
    placed = (
        P(("col", "depth"), "row"),
        P("row", "col"),
        P("row", "col"),
        P("col", "row"),
        P(("col", "depth"), "row"),
    )
    n_row, n_col = mesh.shape["row"], mesh.shape["col"]
    if (n_row, n_col, mesh.shape["depth"]) == (4, 4, 2):
        per_device = functools.partial(grid_device, n_row, n_col)
    else:
        per_device = layered_device
    return jax.shard_map(
        per_device,
        mesh=mesh,
        in_specs=placed,
        out_specs=(
            P(("col", "depth"), "row"),
            P(("row", "depth"), "col"),
            P(("row", "depth"), "col"),
            P(("col", "depth"), "row"),
        ),
        check_vma=False,
    )
```

```python
import functools

import jax
import jax.numpy as jnp
from jax import lax
from jax.experimental import pallas as pl
from jax.experimental.pallas import tpu as pltpu
from jax.sharding import PartitionSpec as P

COLS_CONTRACT = (((1,), (1,)), ((), ()))
ROWS_CONTRACT = (((0,), (0,)), ((), ()))


def gate_grads(hidden_grad, gate_sum, up_sum):
    sigmoid_gate = jax.nn.sigmoid(gate_sum)
    d_gate = (hidden_grad * up_sum * sigmoid_gate * (1.0 + gate_sum * (1.0 - sigmoid_gate))).astype(
        jnp.bfloat16
    )
    d_up = (hidden_grad * gate_sum * sigmoid_gate).astype(jnp.bfloat16)
    return (d_gate, d_up)


def layered_device(tokens, w_gate, w_up, w_down, cotangent):
    hid_width = w_gate.shape[1]
    token_rows = lax.all_gather(tokens, "col", axis=0, tiled=True)
    row_piece = token_rows
    joined = lax.psum_scatter(
        jnp.concatenate(
            [
                jnp.dot(row_piece, w_gate, preferred_element_type=jnp.float32),
                jnp.dot(row_piece, w_up, preferred_element_type=jnp.float32),
            ],
            axis=1,
        ).astype(jnp.bfloat16),
        "row",
        scatter_dimension=0,
        tiled=True,
    ).astype(jnp.float32)
    gate_sum = joined[:, :hid_width]
    up_sum = joined[:, hid_width:]
    hidden = (jax.nn.silu(gate_sum) * up_sum).astype(jnp.bfloat16)
    hidden_rows = lax.all_gather(hidden, "row", axis=0, tiled=True)
    row_piece = hidden_rows
    mixed = lax.psum_scatter(
        jnp.dot(row_piece, w_down, preferred_element_type=jnp.float32).astype(jnp.bfloat16),
        "col",
        scatter_dimension=0,
        tiled=True,
    )
    cot_rows = lax.all_gather(cotangent, "col", axis=0, tiled=True)
    row_piece = cot_rows
    hidden_grad = lax.psum_scatter(
        lax.dot_general(
            row_piece, w_down, COLS_CONTRACT, preferred_element_type=jnp.float32
        ).astype(jnp.bfloat16),
        "row",
        scatter_dimension=0,
        tiled=True,
    ).astype(jnp.float32)
    d_gate, d_up = gate_grads(hidden_grad, gate_sum, up_sum)
    d_gate_rows, d_up_rows = (
        lax.all_gather(d_gate, "row", axis=0, tiled=True),
        lax.all_gather(d_up, "row", axis=0, tiled=True),
    )
    down_term = lax.dot_general(
        hidden_rows, cot_rows, ROWS_CONTRACT, preferred_element_type=jnp.float32
    )
    grad_down = lax.psum_scatter(
        down_term.astype(jnp.bfloat16), "depth", scatter_dimension=0, tiled=True
    )
    layer_tokens = lax.all_to_all(token_rows, "depth", split_axis=1, concat_axis=0, tiled=True)
    block_rows = token_rows.shape[0]
    empty_grad = jnp.zeros((layer_tokens.shape[1], d_gate_rows.shape[1]), jnp.float32)
    first_row = jnp.int32(0)
    gate_total = empty_grad
    up_total = empty_grad
    gate_piece = lax.all_gather(d_gate_rows, "depth", axis=0, tiled=True)
    up_piece = lax.all_gather(d_up_rows, "depth", axis=0, tiled=True)
    for sub_index in range(gate_piece.shape[0] // block_rows):
        gate_block = gate_piece[sub_index * block_rows : (sub_index + 1) * block_rows]
        up_block = up_piece[sub_index * block_rows : (sub_index + 1) * block_rows]
        offset = first_row + sub_index * block_rows
        tok_block = lax.dynamic_slice_in_dim(layer_tokens, offset, block_rows, 0)
        gate_part = lax.optimization_barrier(
            lax.dot_general(
                tok_block, gate_block, ROWS_CONTRACT, preferred_element_type=jnp.float32
            ).astype(jnp.bfloat16)
        )
        up_part = lax.optimization_barrier(
            lax.dot_general(
                tok_block, up_block, ROWS_CONTRACT, preferred_element_type=jnp.float32
            ).astype(jnp.bfloat16)
        )
        gate_total = gate_total + gate_part.astype(jnp.float32)
        up_total = up_total + up_part.astype(jnp.float32)
    return (mixed, gate_total.astype(jnp.bfloat16), up_total.astype(jnp.bfloat16), grad_down)


MESH = pl.DeviceIdType.MESH
VMEM_LIMIT = 52_000_000
VMEM_GRADS = 32_000_000


def f32(x):
    return x.astype(jnp.float32)


def bf16(x):
    return x.astype(jnp.bfloat16)


def rows_dot(x, y):
    return lax.dot_general(x, y, ROWS_CONTRACT, preferred_element_type=jnp.float32)


def exchange_kernel(
    n_row,
    n_col,
    tok_in,
    gate_in,
    up_in,
    down_in,
    cot_in,
    mix_v,
    tok_v,
    tok_far,
    cot_v,
    grad_v,
    hid_v,
    gate_v,
    up_v,
    down_v,
    core_send_v,
    core_recv_v,
    own_v,
    x_send_v,
    x_recv_v,
    mix_acc_v,
    mix_send_v,
    mix_recv_v,
    load_tok_sem,
    load_w_sem,
    z_send,
    z_recv,
    yt_send,
    yt_recv,
    zf_send,
    zf_recv,
    core_send,
    core_recv,
    x_send,
    x_recv,
    near_send,
    near_recv,
    nearh_send,
    nearh_recv,
    y_send,
    y_recv,
    yh_send,
    yh_recv,
    fwd_send,
    fwd_recv,
    fwdh_send,
    fwdh_recv,
    mix_send,
    mix_recv,
):
    row, col, layer = lax.axis_index("row"), lax.axis_index("col"), lax.axis_index("depth")
    core = row % 2
    other = 1 - core
    far_layer = 1 - layer
    blocks, rows, feats = tok_v.shape
    half_feats = tok_far.shape[2]
    quarter = gate_v.shape[2]
    units = x_send_v.shape[0]

    core_id = (row + 1 - 2 * core, col, layer)
    x_id = ((row + 2) % n_row, col, layer)
    y_id = (row, col, far_layer)
    z_ids = {
        1: (row, col + 1 - 2 * (col % 2), layer),
        2: (row, (col + 2) % n_col, layer),
        3: (row, n_col - 1 - col, layer),
    }

    def place(u):
        late, last = (u + units - 3) // units, (u + 1) // units
        second = (u + late) % 2 + last
        return second, (second + far_layer) % 2, (u + late) // 2 - (blocks - 1) * last

    def remote(src, dst, send, recv, device):
        return pltpu.make_async_remote_copy(
            src_ref=src, dst_ref=dst, send_sem=send, recv_sem=recv, device_id=device, device_id_type=MESH
        )

    def load_weight(array, part):
        source = (gate_in, up_in, down_in)[array]
        target = (gate_v, up_v, down_v)[array]
        span = pl.ds(pl.multiple_of(part * quarter, 128), quarter)
        view = source.at[span, :] if array == 2 else source.at[:, span]
        return pltpu.make_async_copy(view, target.at[part], load_w_sem.at[array, part])

    load_tok = pltpu.make_async_copy(tok_in, tok_v.at[0], load_tok_sem.at[0])
    load_cot = pltpu.make_async_copy(cot_in, cot_v.at[0, 0], load_tok_sem.at[1])
    load_tok.start()
    load_cot.start()
    def start_weights(pairs):
        for array, pair in pairs:
            for part in (2 * pair + other, 2 * pair + core):
                load_weight(array, part).start()

    first_q = far_layer
    start_weights([(0, first_q)])

    barrier = pltpu.get_barrier_semaphore()
    peers = [core_id, x_id, y_id] + [z_ids[b] for b in range(1, blocks)]
    for peer in peers:
        pl.semaphore_signal(barrier, inc=1, device_id=peer, device_id_type=MESH)

    def core_copy(u, a):
        return remote(
            core_send_v.at[u, a], core_recv_v.at[u, a], core_send.at[u, a], core_recv.at[u, a], core_id
        )

    def product(u, array, side):
        second, q, b = place(u)
        part = 2 * q + side
        if array == 2:
            return lax.dot_general(
                cot_v[0, b], down_v[part], COLS_CONTRACT, preferred_element_type=jnp.float32
            )
        weight = (gate_v, up_v)[array]
        return jnp.dot(tok_v[b], weight[part], preferred_element_type=jnp.float32)

    load_tok.wait()
    load_weight(0, 2 * first_q + other).wait()
    start_weights([(1, first_q)])
    core_send_v[0, 0] = bf16(product(0, 0, other))
    pl.semaphore_wait(barrier, len(peers))
    core_copy(0, 0).start()

    def z_copy(array, b):
        buffer = (tok_v, cot_v.at[0])[array]
        return remote(buffer.at[0], buffer.at[b], z_send.at[array, b], z_recv.at[array, b], z_ids[b])

    z_copy(0, 1).start()
    load_cot.wait()
    z_copy(1, 1).start()
    for b in range(2, blocks):
        z_copy(0, b).start()
        z_copy(1, b).start()

    def yt_copy(array):
        if array == 0:
            lanes = pl.ds(pl.multiple_of(far_layer * half_feats, 128), half_feats)
            return remote(tok_v.at[0, :, lanes], tok_far.at[0], yt_send.at[0], yt_recv.at[0], y_id)
        return remote(cot_v.at[0, 0], cot_v.at[1, 0], yt_send.at[1], yt_recv.at[1], y_id)

    yt_copy(0).start()
    yt_copy(1).start()

    def zf_copy(array, b):
        buffer = (tok_far, cot_v.at[1])[array]
        return remote(buffer.at[0], buffer.at[b], zf_send.at[array, b], zf_recv.at[array, b], z_ids[b])

    def part_rows(half):
        return pl.ds(half * (rows // 2), rows // 2)

    def x_copy(u, a, half):
        span = part_rows(half)
        return remote(
            x_send_v.at[u, a, span],
            x_recv_v.at[u, a, span],
            x_send.at[u, a, half],
            x_recv.at[u, a, half],
            x_id,
        )

    def near_copy(u, half, side):
        second, q, b = place(u)
        ref = grad_v.at[side, q, :, 0, b, part_rows(half)]
        return remote(ref, ref, near_send.at[u, half], near_recv.at[u, half], core_id)

    def hid_slot(second):
        return 2 - 2 * second

    def nearh_copy(u, half, side):
        second, q, b = place(u)
        ref = hid_v.at[side, hid_slot(second), b, part_rows(half)]
        return remote(ref, ref, nearh_send.at[u, half], nearh_recv.at[u, half], core_id)

    def y_copy(u, half):
        second, q, b = place(u)
        span = part_rows(half)
        return remote(
            grad_v.at[core, q, :, 0, b, span],
            grad_v.at[core, q, :, 1, b, span],
            y_send.at[u, half],
            y_recv.at[u, half],
            y_id,
        )

    def y_arrival(u, half):
        second, q, b = place(u)
        ref = grad_v.at[core, 1 - q, :, 1, b, part_rows(half)]
        return remote(ref, ref, y_send.at[u, half], y_recv.at[u, half], y_id)

    def yh_copy(b, half):
        span = part_rows(half)
        return remote(
            hid_v.at[core, 2, b, span],
            hid_v.at[core, 1, b, span],
            yh_send.at[b, half],
            yh_recv.at[b, half],
            y_id,
        )

    def fwd_copy(u, half, side):
        second, q, b = place(u)
        ref = grad_v.at[side, 1 - q, :, 1, b, part_rows(half)]
        return remote(ref, ref, fwd_send.at[u, half], fwd_recv.at[u, half], core_id)

    def fwdh_copy(b, half, side):
        ref = hid_v.at[side, 1, b, part_rows(half)]
        return remote(ref, ref, fwdh_send.at[b, half], fwdh_recv.at[b, half], core_id)

    def mix_copy(b):
        return remote(mix_send_v.at[b], mix_recv_v.at[b], mix_send.at[b], mix_recv.at[b], z_ids[b])

    def products(u, array):
        def for_other():
            core_send_v[u, array] = bf16(product(u, array, other))
            core_copy(u, array).start()

        if array == 0:
            pl.when(u > 0)(for_other)
        else:
            for_other()
        own_v[u, array] = product(u, array, core)

    def finish(u, array):
        core_copy(u, array).wait_recv()
        total = own_v[u, array] + f32(core_recv_v[u, array])
        own_v[u, array] = total
        x_send_v[u, array] = bf16(total)

        @pl.when(u < units - 1)
        def _():
            for half in range(2):
                x_copy(u, array, half).start()

    def wait_weight(u, array):
        second, q, b = place(u)
        if array == 0:

            @pl.when(u == 1)
            def _():
                load_weight(array, 2 * q + other).wait()
        else:

            @pl.when(b == 0)
            def _():
                load_weight(array, 2 * q + other).wait()

        @pl.when(b == 0)
        def _():
            load_weight(array, 2 * q + core).wait()

    def compute_unit(u):
        second, q, b = place(u)

        for static_b in range(1, blocks):

            @pl.when((b == static_b) & (second == 0))
            def _():
                z_copy(0, static_b).wait_recv()

        wait_weight(u, 0)

        @pl.when(u == 0)
        def _():
            start_weights([(2, first_q)])

        products(u, 0)

        @pl.when(u == 0)
        def _():
            finish(u, 0)

        wait_weight(u, 1)

        @pl.when(u == 0)
        def _():
            start_weights([(0, layer), (1, layer), (2, layer)])

        products(u, 1)

        @pl.when(u > 0)
        def _():
            finish(u, 0)

        for static_b in range(1, blocks):

            @pl.when((b == static_b) & (second == 0))
            def _():
                z_copy(1, static_b).wait_recv()

        wait_weight(u, 2)
        products(u, 2)
        finish(u, 1)
        finish(u, 2)

        @pl.when(u == units - 1)
        def _():
            for half in range(2):
                for array in range(3):
                    x_copy(u, array, half).start()

    row_step = 16

    def over_rows(half, body):
        base = half * (rows // 2)

        def some_rows(i, carry):
            body(pl.ds(pl.multiple_of(base + i * row_step, row_step), row_step))
            return carry

        lax.fori_loop(0, rows // 2 // row_step, some_rows, 0)

    def activate(u, half):
        second, q, b = place(u)
        x_copy(u, 0, half).wait_recv()
        x_copy(u, 1, half).wait_recv()

        def body(span):
            gate_sum = own_v[u, 0, span, :] + f32(x_recv_v[u, 0, span, :])
            up_sum = own_v[u, 1, span, :] + f32(x_recv_v[u, 1, span, :])
            sigmoid_gate = jax.nn.sigmoid(gate_sum)
            swish = gate_sum * sigmoid_gate
            hid_v[core, hid_slot(second), b, span, :] = bf16(swish * up_sum)
            own_v[u, 0, span, :] = up_sum * sigmoid_gate * (1.0 + gate_sum * (1.0 - sigmoid_gate))
            own_v[u, 1, span, :] = swish

        over_rows(half, body)
        nearh_copy(u, half, core).start()

        @pl.when(second == 0)
        def _():
            yh_copy(b, half).start()

    def factors(u, half):
        second, q, b = place(u)
        x_copy(u, 2, half).wait_recv()

        def body(span):
            hidden_grad = own_v[u, 2, span, :] + f32(x_recv_v[u, 2, span, :])
            grad_v[core, q, 0, 0, b, span, :] = bf16(hidden_grad * own_v[u, 0, span, :])
            grad_v[core, q, 1, 0, b, span, :] = bf16(hidden_grad * own_v[u, 1, span, :])

        over_rows(half, body)
        y_copy(u, half).start()
        near_copy(u, half, core).start()

    def elementwise(u):
        for half in range(2):
            activate(u, half)
            factors(u, half)

    def mix_part(u):
        second, q, b = place(u)
        for half in range(2):
            nearh_copy(u, half, other).wait_recv()

        part = jnp.zeros((rows, feats), jnp.float32)
        for side in range(2):
            part = part + jnp.dot(
                hid_v[side, hid_slot(second), b], down_v[2 * q + side], preferred_element_type=jnp.float32
            )

        @pl.when(second == 0)
        def _():
            mix_acc_v[b] = part

        @pl.when((second == 1) & (b == 0))
        def _():
            mix_acc_v[0] = mix_acc_v[0] + part

        @pl.when((second == 1) & (b > 0))
        def _():
            mix_send_v[b] = bf16(mix_acc_v[b] + part)

        for static_b in range(1, blocks):

            @pl.when((second == 1) & (b == static_b))
            def _():
                mix_copy(static_b).start()

    def near_arrived(u):
        for half in range(2):
            near_copy(u, half, other).wait_recv()

        @pl.when(u == 1)
        def _():
            yt_copy(0).wait_recv()
            yt_copy(1).wait_recv()
            for b in range(1, blocks):
                zf_copy(0, b).start()
                zf_copy(1, b).start()

    def far_arrived(u):
        second, q, b = place(u)
        for half in range(2):

            @pl.when(second == 0)
            def _():
                yh_copy(b, half).wait_recv()
                fwdh_copy(b, half, core).start()

            y_arrival(u, half).wait_recv()
            fwd_copy(u, half, core).start()

    def forwarded(u):
        second, q, b = place(u)
        for half in range(2):

            @pl.when(second == 0)
            def _():
                fwdh_copy(b, half, other).wait_recv()

            fwd_copy(u, half, other).wait_recv()

    stages = (
        (elementwise, 2),
        (compute_unit, 0),
        (mix_part, 2),
        (near_arrived, 3),
        (far_arrived, 4),
        (forwarded, 5),
    )

    def step(s, carry):
        for stage, lag in stages:

            @pl.when((s >= lag) & (s < units + lag))
            def _():
                stage(s - lag)

        return carry

    lax.fori_loop(0, units + stages[-1][1], step, 0)

    total = mix_acc_v[0]
    for b in [*range(2, blocks), 1]:
        mix_copy(b).wait_recv()
        total = total + f32(mix_recv_v[b])
    mix_v[...] = bf16(total)

    for b in range(1, blocks):
        zf_copy(0, b).wait_recv()
        zf_copy(1, b).wait_recv()

    for array in range(2):
        yt_copy(array).wait_send()
        for b in range(1, blocks):
            z_copy(array, b).wait_send()
            zf_copy(array, b).wait_send()
    for b in range(1, blocks):
        mix_copy(b).wait_send()

    def drain_block(b, carry):
        for half in range(2):
            yh_copy(b, half).wait_send()
            fwdh_copy(b, half, core).wait_send()
        return carry

    def drain_unit(u, carry):
        for a in range(3):
            core_copy(u, a).wait_send()
        for half in range(2):
            for a in range(3):
                x_copy(u, a, half).wait_send()
            near_copy(u, half, core).wait_send()
            nearh_copy(u, half, core).wait_send()
            y_copy(u, half).wait_send()
            fwd_copy(u, half, core).wait_send()
        return carry

    lax.fori_loop(0, blocks, drain_block, 0)
    lax.fori_loop(0, units, drain_unit, 0)


def gradient_kernel(
    mix_v,
    tok_v,
    tok_far,
    cot_v,
    grad_v,
    hid_v,
    mixed,
    grad_gate,
    grad_up,
    grad_down,
    tok_turned,
    hid_turned,
    wide_v,
    down_v,
    mix_sem,
    wide_sem,
    down_sem,
):
    layer = lax.axis_index("depth")
    blocks, rows, half_feats = tok_far.shape
    half_rows = blocks * rows
    quarter = grad_v.shape[-1]
    mix_copy = pltpu.make_async_copy(mix_v, mixed, mix_sem)
    mix_copy.start()
    own = tok_v[:, :, pl.ds(pl.multiple_of(layer * half_feats, 128), half_feats)]
    tok_turned[:, :half_rows] = own.reshape(half_rows, half_feats).T
    tok_turned[:, half_rows:] = tok_far[...].reshape(half_rows, half_feats).T

    def wide_copy(part, array):
        target = (grad_gate, grad_up)[array]
        lanes = pl.ds(part * quarter, quarter)
        return pltpu.make_async_copy(
            wide_v.at[array, part % 2], target.at[:, lanes], wide_sem.at[array, part % 2]
        )

    def down_copy(part):
        side, half = part // 2, part % 2
        return pltpu.make_async_copy(
            down_v.at[half],
            grad_down.at[pl.ds(side * quarter, quarter), pl.ds(half * half_feats, half_feats)],
            down_sem.at[half],
        )

    for part in range(4):
        q, side = part // 2, part % 2
        for array in range(2):
            if part >= 2:
                wide_copy(part - 2, array).wait()
            factor = grad_v[side, q, array].reshape(2 * half_rows, quarter)
            wide_v[array, part % 2] = bf16(
                jnp.dot(tok_turned[...], factor, preferred_element_type=jnp.float32)
            )
            wide_copy(part, array).start()
        side, half = part // 2, part % 2
        if part >= 2:
            down_copy(part - 2).wait()
        if half == 0:
            hid_turned[...] = hid_v[side, 0:2].reshape(2 * half_rows, quarter).T
        cot = cot_v[:, :, :, half * half_feats : (half + 1) * half_feats]
        down_v[half] = bf16(
            jnp.dot(
                hid_turned[...],
                cot.reshape(2 * half_rows, half_feats),
                preferred_element_type=jnp.float32,
            )
        )
        down_copy(part).start()
    for part in (2, 3):
        wide_copy(part, 0).wait()
        wide_copy(part, 1).wait()
        down_copy(part).wait()
    mix_copy.wait()


def gradients(mixed, tok, tok_far, cot, grad, hid):
    blocks, rows, half_feats = tok_far.shape
    all_rows = 2 * blocks * rows
    feats, quarter = tok.shape[2], grad.shape[-1]
    narrow = jnp.bfloat16
    dma = pltpu.SemaphoreType.DMA
    return pl.pallas_call(
        gradient_kernel,
        out_shape=[
            jax.ShapeDtypeStruct(mixed.shape, narrow),
            jax.ShapeDtypeStruct((half_feats, 4 * quarter), narrow),
            jax.ShapeDtypeStruct((half_feats, 4 * quarter), narrow),
            jax.ShapeDtypeStruct((2 * quarter, feats), narrow),
        ],
        in_specs=[pl.BlockSpec(memory_space=pltpu.VMEM)] * 6,
        out_specs=[pl.BlockSpec(memory_space=pl.ANY)] * 4,
        scratch_shapes=[
            pltpu.VMEM((half_feats, all_rows), narrow),
            pltpu.VMEM((quarter, all_rows), narrow),
            pltpu.VMEM((2, 2, half_feats, quarter), narrow),
            pltpu.VMEM((2, quarter, half_feats), narrow),
            dma,
            dma((2, 2)),
            dma((2,)),
        ],
        compiler_params=pltpu.CompilerParams(vmem_limit_bytes=VMEM_GRADS),
    )(mixed, tok, tok_far, cot, grad, hid)


def grid_device(n_row, n_col, tokens, w_gate, w_up, w_down, cotangent):
    rows, feats = tokens.shape
    hid = w_gate.shape[1]
    quarter = hid // 4
    blocks = n_col
    units = 2 * blocks
    all_rows = 2 * blocks * rows
    narrow, wide = jnp.bfloat16, jnp.float32
    dma = pltpu.SemaphoreType.DMA
    scratch = [
        pltpu.VMEM((4, feats, quarter), narrow),
        pltpu.VMEM((4, feats, quarter), narrow),
        pltpu.VMEM((4, quarter, feats), narrow),
        pltpu.VMEM((units, 3, rows, quarter), narrow),
        pltpu.VMEM((units, 3, rows, quarter), narrow),
        pltpu.VMEM((units, 3, rows, quarter), wide),
        pltpu.VMEM((units, 3, rows, quarter), narrow),
        pltpu.VMEM((units, 3, rows, quarter), narrow),
        pltpu.VMEM((blocks, rows, feats), wide),
        pltpu.VMEM((blocks, rows, feats), narrow),
        pltpu.VMEM((blocks, rows, feats), narrow),
        dma((2,)),
        dma((3, 4)),
        dma((2, blocks)),
        dma((2, blocks)),
        dma((2,)),
        dma((2,)),
        dma((2, blocks)),
        dma((2, blocks)),
        dma((units, 3)),
        dma((units, 3)),
        dma((units, 3, 2)),
        dma((units, 3, 2)),
    ]
    scratch += [dma((units, 2))] * 6
    scratch += [dma((blocks, 2))] * 2
    scratch += [dma((units, 2))] * 2
    scratch += [
        dma((blocks, 2)),
        dma((blocks, 2)),
        dma((blocks,)),
        dma((blocks,)),
    ]
    results = pl.pallas_call(
        functools.partial(exchange_kernel, n_row, n_col),
        out_shape=[
            pltpu.VMEM((rows, feats), narrow),
            pltpu.VMEM((blocks, rows, feats), narrow),
            pltpu.VMEM((blocks, rows, feats // 2), narrow),
            pltpu.VMEM((2, blocks, rows, feats), narrow),
            pltpu.VMEM((2, 2, 2, 2, blocks, rows, quarter), narrow),
            pltpu.VMEM((2, 3, blocks, rows, quarter), narrow),
        ],
        in_specs=[pl.BlockSpec(memory_space=pl.ANY)] * 5,
        out_specs=[pl.BlockSpec(memory_space=pltpu.VMEM)] * 6,
        scratch_shapes=scratch,
        compiler_params=pltpu.CompilerParams(
            collective_id=0, has_side_effects=True, vmem_limit_bytes=VMEM_LIMIT
        ),
    )(tokens, w_gate, w_up, w_down, cotangent)
    return tuple(gradients(*results))


def solution(mesh):
    placed = (
        P(("col", "depth"), "row"),
        P("row", "col"),
        P("row", "col"),
        P("col", "row"),
        P(("col", "depth"), "row"),
    )
    n_row, n_col = mesh.shape["row"], mesh.shape["col"]
    if (n_row, n_col, mesh.shape["depth"]) == (4, 4, 2):
        per_device = functools.partial(grid_device, n_row, n_col)
    else:
        per_device = layered_device
    return jax.shard_map(
        per_device,
        mesh=mesh,
        in_specs=placed,
        out_specs=(
            P(("col", "depth"), "row"),
            P(("row", "depth"), "col"),
            P(("row", "depth"), "col"),
            P(("col", "depth"), "row"),
        ),
        check_vma=False,
    )
```

```python
import functools

import jax
import jax.numpy as jnp
from jax import lax
from jax.experimental import pallas as pl
from jax.experimental.pallas import tpu as pltpu
from jax.sharding import PartitionSpec as P

COLS_CONTRACT = (((1,), (1,)), ((), ()))
ROWS_CONTRACT = (((0,), (0,)), ((), ()))


def gate_grads(hidden_grad, gate_sum, up_sum):
    sigmoid_gate = jax.nn.sigmoid(gate_sum)
    d_gate = (hidden_grad * up_sum * sigmoid_gate * (1.0 + gate_sum * (1.0 - sigmoid_gate))).astype(
        jnp.bfloat16
    )
    d_up = (hidden_grad * gate_sum * sigmoid_gate).astype(jnp.bfloat16)
    return (d_gate, d_up)


def layered_device(tokens, w_gate, w_up, w_down, cotangent):
    hid_width = w_gate.shape[1]
    token_rows = lax.all_gather(tokens, "col", axis=0, tiled=True)
    row_piece = token_rows
    joined = lax.psum_scatter(
        jnp.concatenate(
            [
                jnp.dot(row_piece, w_gate, preferred_element_type=jnp.float32),
                jnp.dot(row_piece, w_up, preferred_element_type=jnp.float32),
            ],
            axis=1,
        ).astype(jnp.bfloat16),
        "row",
        scatter_dimension=0,
        tiled=True,
    ).astype(jnp.float32)
    gate_sum = joined[:, :hid_width]
    up_sum = joined[:, hid_width:]
    hidden = (jax.nn.silu(gate_sum) * up_sum).astype(jnp.bfloat16)
    hidden_rows = lax.all_gather(hidden, "row", axis=0, tiled=True)
    row_piece = hidden_rows
    mixed = lax.psum_scatter(
        jnp.dot(row_piece, w_down, preferred_element_type=jnp.float32).astype(jnp.bfloat16),
        "col",
        scatter_dimension=0,
        tiled=True,
    )
    cot_rows = lax.all_gather(cotangent, "col", axis=0, tiled=True)
    row_piece = cot_rows
    hidden_grad = lax.psum_scatter(
        lax.dot_general(
            row_piece, w_down, COLS_CONTRACT, preferred_element_type=jnp.float32
        ).astype(jnp.bfloat16),
        "row",
        scatter_dimension=0,
        tiled=True,
    ).astype(jnp.float32)
    d_gate, d_up = gate_grads(hidden_grad, gate_sum, up_sum)
    d_gate_rows, d_up_rows = (
        lax.all_gather(d_gate, "row", axis=0, tiled=True),
        lax.all_gather(d_up, "row", axis=0, tiled=True),
    )
    down_term = lax.dot_general(
        hidden_rows, cot_rows, ROWS_CONTRACT, preferred_element_type=jnp.float32
    )
    grad_down = lax.psum_scatter(
        down_term.astype(jnp.bfloat16), "depth", scatter_dimension=0, tiled=True
    )
    layer_tokens = lax.all_to_all(token_rows, "depth", split_axis=1, concat_axis=0, tiled=True)
    block_rows = token_rows.shape[0]
    empty_grad = jnp.zeros((layer_tokens.shape[1], d_gate_rows.shape[1]), jnp.float32)
    first_row = jnp.int32(0)
    gate_total = empty_grad
    up_total = empty_grad
    gate_piece = lax.all_gather(d_gate_rows, "depth", axis=0, tiled=True)
    up_piece = lax.all_gather(d_up_rows, "depth", axis=0, tiled=True)
    for sub_index in range(gate_piece.shape[0] // block_rows):
        gate_block = gate_piece[sub_index * block_rows : (sub_index + 1) * block_rows]
        up_block = up_piece[sub_index * block_rows : (sub_index + 1) * block_rows]
        offset = first_row + sub_index * block_rows
        tok_block = lax.dynamic_slice_in_dim(layer_tokens, offset, block_rows, 0)
        gate_part = lax.optimization_barrier(
            lax.dot_general(
                tok_block, gate_block, ROWS_CONTRACT, preferred_element_type=jnp.float32
            ).astype(jnp.bfloat16)
        )
        up_part = lax.optimization_barrier(
            lax.dot_general(
                tok_block, up_block, ROWS_CONTRACT, preferred_element_type=jnp.float32
            ).astype(jnp.bfloat16)
        )
        gate_total = gate_total + gate_part.astype(jnp.float32)
        up_total = up_total + up_part.astype(jnp.float32)
    return (mixed, gate_total.astype(jnp.bfloat16), up_total.astype(jnp.bfloat16), grad_down)


MESH = pl.DeviceIdType.MESH
VMEM_LIMIT = 50_000_000
VMEM_GRADS = 32_000_000


def f32(x):
    return x.astype(jnp.float32)


def bf16(x):
    return x.astype(jnp.bfloat16)


def rows_dot(x, y):
    return lax.dot_general(x, y, ROWS_CONTRACT, preferred_element_type=jnp.float32)


def exchange_kernel(
    n_row,
    n_col,
    tok_in,
    gate_in,
    up_in,
    down_in,
    cot_in,
    mix_v,
    tok_turned,
    down_grad_v,
    grad_v,
    tok_v,
    tok_far,
    cot_v,
    hid_v,
    hid_turned,
    gate_v,
    up_v,
    down_v,
    core_send_v,
    core_recv_v,
    own_v,
    x_send_v,
    x_recv_v,
    mix_acc_v,
    mix_send_v,
    mix_recv_v,
    load_tok_sem,
    load_w_sem,
    sent,
    late,
    z_recv,
    yt_recv,
    core_recv,
    x_recv,
    nearh_recv,
    y_recv,
    yh_recv,
    mix_recv,
):
    row, col, layer = lax.axis_index("row"), lax.axis_index("col"), lax.axis_index("depth")
    core = row % 2
    other = 1 - core
    far_layer = 1 - layer
    blocks, rows, feats = tok_v.shape
    half_feats = tok_far.shape[2]
    quarter = gate_v.shape[2]
    units = x_send_v.shape[0]

    core_id = (row + 1 - 2 * core, col, layer)
    x_id = ((row + 2) % n_row, col, layer)
    y_id = (row, col, far_layer)
    z_ids = {
        1: (row, col + 1 - 2 * (col % 2), layer),
        2: (row, (col + 2) % n_col, layer),
        3: (row, n_col - 1 - col, layer),
    }

    def place(u):
        skip, final = (u + units - 3) // units, (u + 1) // units
        second = (u + skip) % 2 + final
        return second, (second + far_layer) % 2, (u + skip) // 2 - (blocks - 1) * final

    def remote(src, dst, send, recv, device):
        return pltpu.make_async_remote_copy(
            src_ref=src, dst_ref=dst, send_sem=send, recv_sem=recv, device_id=device, device_id_type=MESH
        )

    def weight_sem(array, second, own):
        if second == 0 and array == 0:
            return load_w_sem.at[own]
        return load_w_sem.at[1 + array + 3 * second]

    def load_weight(array, second):
        for own, side in ((0, other), (1, core)):
            part = 2 * ((second + far_layer) % 2) + side
            source = (gate_in, up_in, down_in)[array]
            target = (gate_v, up_v, down_v)[array]
            span = pl.ds(pl.multiple_of(part * quarter, 128), quarter)
            view = source.at[span, :] if array == 2 else source.at[:, span]
            pltpu.make_async_copy(view, target.at[part], weight_sem(array, second, own)).start()

    def weight_wait(array, second, own):
        source = (gate_in, up_in, down_in)[array]
        target = (gate_v, up_v, down_v)[array]
        single = second == 0 and array == 0
        wide = quarter if single else 2 * quarter
        view = source.at[0:wide, :] if array == 2 else source.at[:, 0:wide]
        pltpu.make_async_copy(view, view, weight_sem(array, second, own)).wait()

    load_tok = pltpu.make_async_copy(tok_in, tok_v.at[0], load_tok_sem.at[0])
    load_cot = pltpu.make_async_copy(cot_in, cot_v.at[0, 0], load_tok_sem.at[1])
    load_tok.start()
    load_cot.start()
    load_weight(0, 0)

    barrier = pltpu.get_barrier_semaphore()
    peers = [core_id, x_id, y_id] + [z_ids[b] for b in range(1, blocks)]
    for peer in peers:
        pl.semaphore_signal(barrier, inc=1, device_id=peer, device_id_type=MESH)

    def core_copy(u, a):
        return remote(
            core_send_v.at[u, a], core_recv_v.at[u, a], sent.at[0], core_recv.at[u, a], core_id
        )

    def product(u, array, side):
        second, q, b = place(u)
        part = 2 * q + side
        if array == 2:
            return lax.dot_general(
                cot_v[0, b], down_v[part], COLS_CONTRACT, preferred_element_type=jnp.float32
            )
        weight = (gate_v, up_v)[array]
        return jnp.dot(tok_v[b], weight[part], preferred_element_type=jnp.float32)

    load_tok.wait()
    weight_wait(0, 0, 0)
    load_weight(1, 0)
    core_send_v[0, 0] = bf16(product(0, 0, other))
    pl.semaphore_wait(barrier, len(peers))
    core_copy(0, 0).start()

    def z_copy(array, b):
        buffer = (tok_v, cot_v.at[0])[array]
        return remote(buffer.at[0], buffer.at[b], sent.at[1 + array], z_recv.at[array, b], z_ids[b])

    z_copy(0, 1).start()
    load_cot.wait()
    z_copy(1, 1).start()
    for b in range(2, blocks):
        z_copy(0, b).start()
        z_copy(1, b).start()

    def yt_copy(array):
        if array == 0:
            lanes = pl.ds(pl.multiple_of(far_layer * half_feats, 128), half_feats)
            return remote(tok_v.at[0, :, lanes], tok_far.at[0], sent.at[3], yt_recv.at[0], y_id)
        return remote(cot_v.at[0, 0], cot_v.at[1, 0], sent.at[4], yt_recv.at[1], y_id)

    yt_copy(0).start()
    yt_copy(1).start()

    def zf_copy(array, b):
        buffer = (tok_far, cot_v.at[1])[array]
        return remote(buffer.at[0], buffer.at[b], sent.at[5 + array], late.at[array], z_ids[b])

    def part_rows(half):
        return pl.ds(half * (rows // 2), rows // 2)

    def x_copy(u, a, half):
        span = part_rows(half)
        return remote(
            x_send_v.at[u, a, span],
            x_recv_v.at[u, a, span],
            sent.at[7],
            x_recv.at[u, a // 2, half],
            x_id,
        )

    def x_pair_arrival(u, half):
        ref = x_recv_v.at[u, 0:2, part_rows(half)]
        return remote(ref, ref, sent.at[7], x_recv.at[u, 0, half], x_id)

    def near_copy(u, half):
        second, q, b = place(u)
        ref = grad_v.at[core, q, :, 0, b, part_rows(half)]
        return remote(ref, ref, sent.at[8], late.at[2], core_id)

    def hid_slot(second):
        return 2 - 2 * second

    def nearh_copy(u, half):
        second, q, b = place(u)
        ref = hid_v.at[core, hid_slot(second), b, part_rows(half)]
        return remote(ref, ref, sent.at[9], nearh_recv.at[u], core_id)

    def nearh_arrival(u):
        second, q, b = place(u)
        ref = hid_v.at[other, hid_slot(second), b]
        return remote(ref, ref, sent.at[9], nearh_recv.at[u], core_id)

    def y_slot(u, half):
        return u + half * ((u + 1) // units)

    def y_copy(u, half):
        second, q, b = place(u)
        span = part_rows(half)
        return remote(
            grad_v.at[core, q, :, 0, b, span],
            grad_v.at[core, q, :, 1, b, span],
            sent.at[10],
            y_recv.at[y_slot(u, half)],
            y_id,
        )

    def y_arrival(u, span, slot):
        second, q, b = place(u)
        ref = grad_v.at[core, 1 - q, :, 1, b, span]
        return remote(ref, ref, sent.at[10], y_recv.at[slot], y_id)

    def yh_copy(b, half):
        span = part_rows(half)
        return remote(
            hid_v.at[core, 2, b, span], hid_v.at[core, 1, b, span], sent.at[11], yh_recv.at[b], y_id
        )

    def yh_arrival(b):
        ref = hid_v.at[core, 1, b]
        return remote(ref, ref, sent.at[11], yh_recv.at[b], y_id)

    def fwd_copy(u, span):
        second, q, b = place(u)
        ref = grad_v.at[core, 1 - q, :, 1, b, span]
        return remote(ref, ref, sent.at[12], late.at[3], core_id)

    def fwdh_copy(b):
        ref = hid_v.at[core, 1, b]
        return remote(ref, ref, sent.at[13], late.at[4], core_id)

    def mix_copy(b):
        return remote(mix_send_v.at[b], mix_recv_v.at[b], sent.at[14], mix_recv.at[b], z_ids[b])

    def all_sent(ref, slot):
        remote(ref, ref, sent.at[slot], late.at[0], core_id).wait_send()

    def all_arrived(ref, slot):
        remote(ref, ref, sent.at[0], late.at[slot], core_id).wait_recv()

    def products(u, array):
        def for_other():
            core_send_v[u, array] = bf16(product(u, array, other))
            core_copy(u, array).start()

        if array == 0:
            pl.when(u > 0)(for_other)
        else:
            for_other()
        own_v[u, array] = product(u, array, core)

    def finish(u, array):
        core_copy(u, array).wait_recv()
        total = own_v[u, array] + f32(core_recv_v[u, array])
        own_v[u, array] = total
        x_send_v[u, array] = bf16(total)

        @pl.when(u < units - 1)
        def _():
            for half in range(2):
                x_copy(u, array, half).start()

    def wait_weight(u, array):
        for second in range(2):

            @pl.when(u == second)
            def _():
                weight_wait(array, second, 1)

    def compute_unit(u):
        second, q, b = place(u)

        for static_b in range(1, blocks):

            @pl.when((b == static_b) & (second == 0))
            def _():
                z_copy(0, static_b).wait_recv()

        wait_weight(u, 0)

        @pl.when(u == 0)
        def _():
            load_weight(2, 0)

        products(u, 0)

        @pl.when(u == 0)
        def _():
            finish(u, 0)

        wait_weight(u, 1)

        @pl.when(u == 0)
        def _():
            for array in range(3):
                load_weight(array, 1)

        products(u, 1)

        @pl.when(u > 0)
        def _():
            finish(u, 0)

        for static_b in range(1, blocks):

            @pl.when((b == static_b) & (second == 0))
            def _():
                z_copy(1, static_b).wait_recv()

        wait_weight(u, 2)
        products(u, 2)
        finish(u, 1)
        finish(u, 2)

        @pl.when(u == units - 1)
        def _():
            for half in range(2):
                for array in range(3):
                    x_copy(u, array, half).start()

    row_step = 16

    def over_rows(half, body):
        base = half * (rows // 2)

        def some_rows(i, carry):
            body(pl.ds(pl.multiple_of(base + i * row_step, row_step), row_step))
            return carry

        lax.fori_loop(0, rows // 2 // row_step, some_rows, 0)

    def activate(u, half):
        second, q, b = place(u)
        x_pair_arrival(u, half).wait_recv()

        def body(span):
            gate_sum = own_v[u, 0, span, :] + f32(x_recv_v[u, 0, span, :])
            up_sum = own_v[u, 1, span, :] + f32(x_recv_v[u, 1, span, :])
            sigmoid_gate = jax.nn.sigmoid(gate_sum)
            swish = gate_sum * sigmoid_gate
            hid_v[core, hid_slot(second), b, span, :] = bf16(swish * up_sum)
            own_v[u, 0, span, :] = up_sum * sigmoid_gate * (1.0 + gate_sum * (1.0 - sigmoid_gate))
            own_v[u, 1, span, :] = swish

        over_rows(half, body)
        nearh_copy(u, half).start()

        @pl.when(second == 0)
        def _():
            yh_copy(b, half).start()

    def factors(u, half):
        second, q, b = place(u)
        x_copy(u, 2, half).wait_recv()

        def body(span):
            hidden_grad = own_v[u, 2, span, :] + f32(x_recv_v[u, 2, span, :])
            grad_v[core, q, 0, 0, b, span, :] = bf16(hidden_grad * own_v[u, 0, span, :])
            grad_v[core, q, 1, 0, b, span, :] = bf16(hidden_grad * own_v[u, 1, span, :])

        over_rows(half, body)
        y_copy(u, half).start()
        near_copy(u, half).start()

    def elementwise(u):
        for half in range(2):
            activate(u, half)
            factors(u, half)

    def mix_part(u):
        second, q, b = place(u)
        nearh_arrival(u).wait_recv()

        part = jnp.zeros((rows, feats), jnp.float32)
        for side in range(2):
            part = part + jnp.dot(
                hid_v[side, hid_slot(second), b], down_v[2 * q + side], preferred_element_type=jnp.float32
            )

        @pl.when(second == 0)
        def _():
            mix_acc_v[b] = part

        @pl.when((second == 1) & (b == 0))
        def _():
            mix_acc_v[0] = mix_acc_v[0] + part

        @pl.when((second == 1) & (b > 0))
        def _():
            mix_send_v[b] = bf16(mix_acc_v[b] + part)

        for static_b in range(1, blocks):

            @pl.when((second == 1) & (b == static_b))
            def _():
                mix_copy(static_b).start()

    def spread_far():
        yt_copy(0).wait_recv()
        yt_copy(1).wait_recv()
        for b in range(1, blocks):
            zf_copy(0, b).start()
            zf_copy(1, b).start()

    def far_arrived(u):
        second, q, b = place(u)

        @pl.when(second == 0)
        def _():
            yh_arrival(b).wait_recv()
            fwdh_copy(b).start()

        whole = pl.ds(0, rows)
        y_arrival(u, whole, u).wait_recv()
        fwd_copy(u, whole).start()

    def last_far(half):
        span = part_rows(half)
        y_arrival(units - 1, span, units - 1 + half).wait_recv()
        fwd_copy(units - 1, span).start()

    def turn_tokens():
        all_arrived(tok_far.at[1:blocks], 0)
        all_arrived(cot_v.at[1, 1:blocks], 1)
        half_rows = blocks * rows
        own = tok_v[:, :, pl.ds(pl.multiple_of(layer * half_feats, 128), half_feats)]
        tok_turned[:, :half_rows] = own.reshape(half_rows, half_feats).T
        tok_turned[:, half_rows:] = tok_far[...].reshape(half_rows, half_feats).T

    def down_grad(side, half):
        if half == 0:
            hid_turned[...] = hid_v[side, 0:2].reshape(2 * blocks * rows, quarter).T
        lanes = slice(half * half_feats, (half + 1) * half_feats)
        down_grad_v[side * quarter : (side + 1) * quarter, lanes] = bf16(
            jnp.dot(
                hid_turned[...],
                cot_v[:, :, :, lanes].reshape(2 * blocks * rows, half_feats),
                preferred_element_type=jnp.float32,
            )
        )

    stages = ((elementwise, 2), (compute_unit, 0), (mix_part, 2), (far_arrived, 4))

    def step(s, carry):
        for stage, lag in stages:

            @pl.when((s >= lag) & (s < units + lag))
            def _():
                stage(s - lag)

        pl.when(s == 4)(spread_far)
        pl.when(s == units)(turn_tokens)
        return carry

    lax.fori_loop(0, units + 2, step, 0)
    far_arrived(units - 2)
    all_arrived(hid_v.at[other, 1], 4)
    down_grad(0, 0)
    last_far(0)
    down_grad(0, 1)
    down_grad(1, 0)
    last_far(1)
    down_grad(1, 1)

    total = mix_acc_v[0]
    for b in [*range(2, blocks), 1]:
        mix_copy(b).wait_recv()
        total = total + f32(mix_recv_v[b])
    mix_v[...] = bf16(total)

    all_arrived(grad_v.at[other, :, :, 0], 2)
    all_arrived(grad_v.at[other, :, :, 1], 3)
    all_sent(core_send_v, 0)
    all_sent(tok_v.at[1:blocks], 1)
    all_sent(cot_v.at[0, 1:blocks], 2)
    all_sent(tok_far.at[0], 3)
    all_sent(cot_v.at[0, 0], 4)
    all_sent(tok_far.at[1:blocks], 5)
    all_sent(cot_v.at[1, 1:blocks], 6)
    all_sent(x_send_v, 7)
    all_sent(grad_v.at[core, :, :, 0], 8)
    all_sent(hid_v.at[core, 0:2], 9)
    all_sent(grad_v.at[core, :, :, 0], 10)
    all_sent(hid_v.at[core, 2], 11)
    all_sent(grad_v.at[core, :, :, 1], 12)
    all_sent(hid_v.at[core, 1], 13)
    all_sent(mix_send_v.at[1:blocks], 14)


def gradient_kernel(
    mix_v, tok_turned, down_grad_v, grad_v, mixed, grad_gate, grad_up, grad_down, wide_v, done, wide_sem
):
    quarter = grad_v.shape[-1]
    all_rows = tok_turned.shape[1]
    mix_copy = pltpu.make_async_copy(mix_v, mixed, done.at[0])
    down_copy = pltpu.make_async_copy(down_grad_v, grad_down, done.at[1])
    mix_copy.start()
    down_copy.start()
    copies = []
    for part in range(4):
        q, side = part // 2, part % 2
        for array in range(2):
            slot = len(copies) % 4
            if len(copies) >= 4:
                copies[-4].wait()
            factor = grad_v[side, q, array].reshape(all_rows, quarter)
            wide_v[slot] = bf16(jnp.dot(tok_turned[...], factor, preferred_element_type=jnp.float32))
            target = (grad_gate, grad_up)[array]
            copies.append(
                pltpu.make_async_copy(
                    wide_v.at[slot], target.at[:, pl.ds(part * quarter, quarter)], wide_sem.at[slot]
                )
            )
            copies[-1].start()
    for copy in copies[-4:]:
        copy.wait()
    mix_copy.wait()
    down_copy.wait()


def gradients(mixed, tok, down_grad, grad):
    half_feats, quarter = tok.shape[0], grad.shape[-1]
    narrow = jnp.bfloat16
    dma = pltpu.SemaphoreType.DMA
    return pl.pallas_call(
        gradient_kernel,
        out_shape=[
            jax.ShapeDtypeStruct(mixed.shape, narrow),
            jax.ShapeDtypeStruct((half_feats, 4 * quarter), narrow),
            jax.ShapeDtypeStruct((half_feats, 4 * quarter), narrow),
            jax.ShapeDtypeStruct(down_grad.shape, narrow),
        ],
        in_specs=[pl.BlockSpec(memory_space=pltpu.VMEM)] * 4,
        out_specs=[pl.BlockSpec(memory_space=pl.ANY)] * 4,
        scratch_shapes=[pltpu.VMEM((4, half_feats, quarter), narrow), dma((2,)), dma((4,))],
        compiler_params=pltpu.CompilerParams(vmem_limit_bytes=VMEM_GRADS),
    )(mixed, tok, down_grad, grad)


def grid_device(n_row, n_col, tokens, w_gate, w_up, w_down, cotangent):
    rows, feats = tokens.shape
    hid = w_gate.shape[1]
    quarter = hid // 4
    blocks = n_col
    units = 2 * blocks
    all_rows = 2 * blocks * rows
    narrow, wide = jnp.bfloat16, jnp.float32
    dma = pltpu.SemaphoreType.DMA
    results = pl.pallas_call(
        functools.partial(exchange_kernel, n_row, n_col),
        out_shape=[
            pltpu.VMEM((rows, feats), narrow),
            pltpu.VMEM((feats // 2, all_rows), narrow),
            pltpu.VMEM((hid // 2, feats), narrow),
            pltpu.VMEM((2, 2, 2, 2, blocks, rows, quarter), narrow),
        ],
        in_specs=[pl.BlockSpec(memory_space=pl.ANY)] * 5,
        out_specs=[pl.BlockSpec(memory_space=pltpu.VMEM)] * 4,
        scratch_shapes=[
            pltpu.VMEM((blocks, rows, feats), narrow),
            pltpu.VMEM((blocks, rows, feats // 2), narrow),
            pltpu.VMEM((2, blocks, rows, feats), narrow),
            pltpu.VMEM((2, 3, blocks, rows, quarter), narrow),
            pltpu.VMEM((quarter, all_rows), narrow),
            pltpu.VMEM((4, feats, quarter), narrow),
            pltpu.VMEM((4, feats, quarter), narrow),
            pltpu.VMEM((4, quarter, feats), narrow),
            pltpu.VMEM((units, 3, rows, quarter), narrow),
            pltpu.VMEM((units, 3, rows, quarter), narrow),
            pltpu.VMEM((units, 3, rows, quarter), wide),
            pltpu.VMEM((units, 3, rows, quarter), narrow),
            pltpu.VMEM((units, 3, rows, quarter), narrow),
            pltpu.VMEM((blocks, rows, feats), wide),
            pltpu.VMEM((blocks, rows, feats), narrow),
            pltpu.VMEM((blocks, rows, feats), narrow),
            dma((2,)),
            dma((7,)),
            dma((15,)),
            dma((5,)),
            dma((2, blocks)),
            dma((2,)),
            dma((units, 3)),
            dma((units, 2, 2)),
            dma((units,)),
            dma((units + 1,)),
            dma((blocks,)),
            dma((blocks,)),
        ],
        compiler_params=pltpu.CompilerParams(
            collective_id=0, has_side_effects=True, vmem_limit_bytes=VMEM_LIMIT
        ),
    )(tokens, w_gate, w_up, w_down, cotangent)
    return tuple(gradients(*results))


def solution(mesh):
    placed = (
        P(("col", "depth"), "row"),
        P("row", "col"),
        P("row", "col"),
        P("col", "row"),
        P(("col", "depth"), "row"),
    )
    n_row, n_col = mesh.shape["row"], mesh.shape["col"]
    if (n_row, n_col, mesh.shape["depth"]) == (4, 4, 2):
        per_device = functools.partial(grid_device, n_row, n_col)
    else:
        per_device = layered_device
    return jax.shard_map(
        per_device,
        mesh=mesh,
        in_specs=placed,
        out_specs=(
            P(("col", "depth"), "row"),
            P(("row", "depth"), "col"),
            P(("row", "depth"), "col"),
            P(("col", "depth"), "row"),
        ),
        check_vma=False,
    )
```

```python
import functools

import jax
import jax.numpy as jnp
from jax import lax
from jax.experimental import pallas as pl
from jax.experimental.pallas import tpu as pltpu
from jax.sharding import PartitionSpec as P

COLS_CONTRACT = (((1,), (1,)), ((), ()))
ROWS_CONTRACT = (((0,), (0,)), ((), ()))


def gate_grads(hidden_grad, gate_sum, up_sum):
    sigmoid_gate = jax.nn.sigmoid(gate_sum)
    d_gate = (hidden_grad * up_sum * sigmoid_gate * (1.0 + gate_sum * (1.0 - sigmoid_gate))).astype(
        jnp.bfloat16
    )
    d_up = (hidden_grad * gate_sum * sigmoid_gate).astype(jnp.bfloat16)
    return (d_gate, d_up)


def layered_device(tokens, w_gate, w_up, w_down, cotangent):
    hid_width = w_gate.shape[1]
    token_rows = lax.all_gather(tokens, "col", axis=0, tiled=True)
    row_piece = token_rows
    joined = lax.psum_scatter(
        jnp.concatenate(
            [
                jnp.dot(row_piece, w_gate, preferred_element_type=jnp.float32),
                jnp.dot(row_piece, w_up, preferred_element_type=jnp.float32),
            ],
            axis=1,
        ).astype(jnp.bfloat16),
        "row",
        scatter_dimension=0,
        tiled=True,
    ).astype(jnp.float32)
    gate_sum = joined[:, :hid_width]
    up_sum = joined[:, hid_width:]
    hidden = (jax.nn.silu(gate_sum) * up_sum).astype(jnp.bfloat16)
    hidden_rows = lax.all_gather(hidden, "row", axis=0, tiled=True)
    row_piece = hidden_rows
    mixed = lax.psum_scatter(
        jnp.dot(row_piece, w_down, preferred_element_type=jnp.float32).astype(jnp.bfloat16),
        "col",
        scatter_dimension=0,
        tiled=True,
    )
    cot_rows = lax.all_gather(cotangent, "col", axis=0, tiled=True)
    row_piece = cot_rows
    hidden_grad = lax.psum_scatter(
        lax.dot_general(
            row_piece, w_down, COLS_CONTRACT, preferred_element_type=jnp.float32
        ).astype(jnp.bfloat16),
        "row",
        scatter_dimension=0,
        tiled=True,
    ).astype(jnp.float32)
    d_gate, d_up = gate_grads(hidden_grad, gate_sum, up_sum)
    d_gate_rows, d_up_rows = (
        lax.all_gather(d_gate, "row", axis=0, tiled=True),
        lax.all_gather(d_up, "row", axis=0, tiled=True),
    )
    down_term = lax.dot_general(
        hidden_rows, cot_rows, ROWS_CONTRACT, preferred_element_type=jnp.float32
    )
    grad_down = lax.psum_scatter(
        down_term.astype(jnp.bfloat16), "depth", scatter_dimension=0, tiled=True
    )
    layer_tokens = lax.all_to_all(token_rows, "depth", split_axis=1, concat_axis=0, tiled=True)
    block_rows = token_rows.shape[0]
    empty_grad = jnp.zeros((layer_tokens.shape[1], d_gate_rows.shape[1]), jnp.float32)
    first_row = jnp.int32(0)
    gate_total = empty_grad
    up_total = empty_grad
    gate_piece = lax.all_gather(d_gate_rows, "depth", axis=0, tiled=True)
    up_piece = lax.all_gather(d_up_rows, "depth", axis=0, tiled=True)
    for sub_index in range(gate_piece.shape[0] // block_rows):
        gate_block = gate_piece[sub_index * block_rows : (sub_index + 1) * block_rows]
        up_block = up_piece[sub_index * block_rows : (sub_index + 1) * block_rows]
        offset = first_row + sub_index * block_rows
        tok_block = lax.dynamic_slice_in_dim(layer_tokens, offset, block_rows, 0)
        gate_part = lax.optimization_barrier(
            lax.dot_general(
                tok_block, gate_block, ROWS_CONTRACT, preferred_element_type=jnp.float32
            ).astype(jnp.bfloat16)
        )
        up_part = lax.optimization_barrier(
            lax.dot_general(
                tok_block, up_block, ROWS_CONTRACT, preferred_element_type=jnp.float32
            ).astype(jnp.bfloat16)
        )
        gate_total = gate_total + gate_part.astype(jnp.float32)
        up_total = up_total + up_part.astype(jnp.float32)
    return (mixed, gate_total.astype(jnp.bfloat16), up_total.astype(jnp.bfloat16), grad_down)


MESH = pl.DeviceIdType.MESH
VMEM_LIMIT = 50_000_000
VMEM_GRADS = 32_000_000


def f32(x):
    return x.astype(jnp.float32)


def bf16(x):
    return x.astype(jnp.bfloat16)


def rows_dot(x, y):
    return lax.dot_general(x, y, ROWS_CONTRACT, preferred_element_type=jnp.float32)


def exchange_kernel(
    n_row,
    n_col,
    tok_in,
    gate_in,
    up_in,
    down_in,
    cot_in,
    mix_v,
    tok_turned,
    down_grad_v,
    grad_v,
    tok_v,
    tok_far,
    cot_v,
    hid_v,
    hid_turned,
    gate_v,
    up_v,
    down_v,
    core_send_v,
    core_recv_v,
    own_v,
    x_send_v,
    x_recv_v,
    mix_acc_v,
    mix_send_v,
    mix_recv_v,
    load_tok_sem,
    load_w_sem,
    sent,
    late,
    z_recv,
    yt_recv,
    core_recv,
    x_recv,
    x_last,
    nearh_recv,
    y_recv,
    yh_recv,
    mix_recv,
):
    row, col, layer = lax.axis_index("row"), lax.axis_index("col"), lax.axis_index("depth")
    core = row % 2
    other = 1 - core
    far_layer = 1 - layer
    blocks, rows, feats = tok_v.shape
    half_feats = tok_far.shape[2]
    quarter = gate_v.shape[2]
    units = x_send_v.shape[0]

    core_lanes = pl.ds(pl.multiple_of(core * quarter, 128), quarter)
    other_lanes = pl.ds(pl.multiple_of(other * quarter, 128), quarter)

    core_id = (row + 1 - 2 * core, col, layer)
    x_id = ((row + 2) % n_row, col, layer)
    y_id = (row, col, far_layer)
    z_ids = {
        1: (row, col + 1 - 2 * (col % 2), layer),
        2: (row, (col + 2) % n_col, layer),
        3: (row, n_col - 1 - col, layer),
    }

    def place(u):
        skip, final = (u + units - 3) // units, (u + 1) // units
        second = (u + skip) % 2 + final
        return second, (second + far_layer) % 2, (u + skip) // 2 - (blocks - 1) * final

    def remote(src, dst, send, recv, device):
        return pltpu.make_async_remote_copy(
            src_ref=src, dst_ref=dst, send_sem=send, recv_sem=recv, device_id=device, device_id_type=MESH
        )

    def weight_sem(array, second, own):
        if second == 0 and array == 0:
            return load_w_sem.at[own]
        return load_w_sem.at[1 + array + 3 * second]

    def load_weight(array, second):
        for own, side in ((0, other), (1, core)):
            part = 2 * ((second + far_layer) % 2) + side
            source = (gate_in, up_in, down_in)[array]
            target = (gate_v, up_v, down_v)[array]
            span = pl.ds(pl.multiple_of(part * quarter, 128), quarter)
            view = source.at[span, :] if array == 2 else source.at[:, span]
            pltpu.make_async_copy(view, target.at[part], weight_sem(array, second, own)).start()

    def weight_wait(array, second, own):
        source = (gate_in, up_in, down_in)[array]
        target = (gate_v, up_v, down_v)[array]
        single = second == 0 and array == 0
        wide = quarter if single else 2 * quarter
        view = source.at[0:wide, :] if array == 2 else source.at[:, 0:wide]
        pltpu.make_async_copy(view, view, weight_sem(array, second, own)).wait()

    load_tok = pltpu.make_async_copy(tok_in, tok_v.at[0], load_tok_sem.at[0])
    load_cot = pltpu.make_async_copy(cot_in, cot_v.at[0, 0], load_tok_sem.at[1])
    load_tok.start()
    load_cot.start()
    load_weight(0, 0)

    barrier = pltpu.get_barrier_semaphore()
    peers = [core_id, x_id, y_id] + [z_ids[b] for b in range(1, blocks)]
    for peer in peers:
        pl.semaphore_signal(barrier, inc=1, device_id=peer, device_id_type=MESH)

    def core_copy(u, a):
        return remote(
            core_send_v.at[u, a], core_recv_v.at[u, a], sent.at[0], core_recv.at[u, a], core_id
        )

    def product(u, array, side):
        second, q, b = place(u)
        part = 2 * q + side
        if array == 2:
            return lax.dot_general(
                cot_v[0, b], down_v[part], COLS_CONTRACT, preferred_element_type=jnp.float32
            )
        weight = (gate_v, up_v)[array]
        return jnp.dot(tok_v[b], weight[part], preferred_element_type=jnp.float32)

    load_tok.wait()
    weight_wait(0, 0, 0)
    load_weight(1, 0)
    core_send_v[0, 0] = bf16(product(0, 0, other))
    pl.semaphore_wait(barrier, len(peers))
    core_copy(0, 0).start()

    def z_copy(array, b):
        buffer = (tok_v, cot_v.at[0])[array]
        return remote(buffer.at[0], buffer.at[b], sent.at[1 + array], z_recv.at[array, b], z_ids[b])

    z_copy(0, 1).start()
    load_cot.wait()
    z_copy(1, 1).start()
    for b in range(2, blocks):
        z_copy(0, b).start()
        z_copy(1, b).start()

    def yt_copy(array):
        if array == 0:
            lanes = pl.ds(pl.multiple_of(far_layer * half_feats, 128), half_feats)
            return remote(tok_v.at[0, :, lanes], tok_far.at[0], sent.at[3], yt_recv.at[0], y_id)
        return remote(cot_v.at[0, 0], cot_v.at[1, 0], sent.at[4], yt_recv.at[1], y_id)

    yt_copy(0).start()
    yt_copy(1).start()

    def zf_copy(array, b):
        buffer = (tok_far, cot_v.at[1])[array]
        return remote(buffer.at[0], buffer.at[b], sent.at[5 + array], late.at[array], z_ids[b])

    last = units - 1
    halves, pieces = 2, 4

    def part_rows(part, parts):
        return pl.ds(part * (rows // parts), rows // parts)

    def x_copy(u, a, span, recv):
        return remote(x_send_v.at[u, a, span], x_recv_v.at[u, a, span], sent.at[7], recv, x_id)

    def x_sem(u, a, part):
        return x_recv.at[u, a // 2, part]

    def x_last_sem(a, part):
        return x_last.at[a // 2, part]

    def x_pair_arrival(u, span, recv):
        ref = x_recv_v.at[u, 0:2, span]
        return remote(ref, ref, sent.at[7], recv, x_id)

    def near_copy(u, span):
        second, q, b = place(u)
        ref = grad_v.at[q, :, 0, b, span, core_lanes]
        return remote(ref, ref, sent.at[8], late.at[2], core_id)

    def hid_slot(second):
        return 2 - 2 * second

    def nearh_copy(u, span, slot, side):
        second, q, b = place(u)
        ref = hid_v.at[side, hid_slot(second), b, span]
        return remote(ref, ref, sent.at[9], nearh_recv.at[slot], core_id)

    def y_copy(u, span, slot):
        second, q, b = place(u)
        return remote(
            grad_v.at[q, :, 0, b, span, core_lanes],
            grad_v.at[q, :, 1, b, span, core_lanes],
            sent.at[10],
            y_recv.at[slot],
            y_id,
        )

    def y_arrival(u, span, slot):
        second, q, b = place(u)
        ref = grad_v.at[1 - q, :, 1, b, span, core_lanes]
        return remote(ref, ref, sent.at[10], y_recv.at[slot], y_id)

    def yh_copy(b, span):
        return remote(
            hid_v.at[core, 2, b, span], hid_v.at[core, 1, b, span], sent.at[11], yh_recv.at[b], y_id
        )

    def yh_arrival(b):
        ref = hid_v.at[core, 1, b]
        return remote(ref, ref, sent.at[11], yh_recv.at[b], y_id)

    def fwd_copy(u, span):
        second, q, b = place(u)
        ref = grad_v.at[1 - q, :, 1, b, span, core_lanes]
        return remote(ref, ref, sent.at[12], late.at[3], core_id)

    def fwdh_copy(b):
        ref = hid_v.at[core, 1, b]
        return remote(ref, ref, sent.at[13], late.at[4], core_id)

    def mix_copy(b):
        return remote(mix_send_v.at[b], mix_recv_v.at[b], sent.at[14], mix_recv.at[b], z_ids[b])

    def mix_last_copy(half):
        span = part_rows(half, halves)
        return remote(
            mix_send_v.at[1, span], mix_recv_v.at[1, span], sent.at[14], mix_recv.at[half], z_ids[1]
        )

    def all_sent(ref, slot):
        remote(ref, ref, sent.at[slot], late.at[0], core_id).wait_send()

    def all_arrived(ref, slot):
        remote(ref, ref, sent.at[0], late.at[slot], core_id).wait_recv()

    def products(u, array):
        def for_other():
            core_send_v[u, array] = bf16(product(u, array, other))
            core_copy(u, array).start()

        if array == 0:
            pl.when(u > 0)(for_other)
        else:
            for_other()
        own_v[u, array] = product(u, array, core)

    def finish(u, array):
        core_copy(u, array).wait_recv()
        total = own_v[u, array] + f32(core_recv_v[u, array])
        own_v[u, array] = total
        x_send_v[u, array] = bf16(total)

        @pl.when(u < last)
        def _():
            for half in range(halves):
                x_copy(u, array, part_rows(half, halves), x_sem(u, array, half)).start()

    def wait_weight(u, array):
        for second in range(2):

            @pl.when(u == second)
            def _():
                weight_wait(array, second, 1)

    def compute_unit(u):
        second, q, b = place(u)

        for static_b in range(1, blocks):

            @pl.when((b == static_b) & (second == 0))
            def _():
                z_copy(0, static_b).wait_recv()

        wait_weight(u, 0)

        @pl.when(u == 0)
        def _():
            load_weight(2, 0)

        products(u, 0)

        @pl.when(u == 0)
        def _():
            finish(u, 0)

        wait_weight(u, 1)

        @pl.when(u == 0)
        def _():
            for array in range(3):
                load_weight(array, 1)

        products(u, 1)

        @pl.when(u > 0)
        def _():
            finish(u, 0)

        for static_b in range(1, blocks):

            @pl.when((b == static_b) & (second == 0))
            def _():
                z_copy(1, static_b).wait_recv()

        wait_weight(u, 2)
        products(u, 2)
        finish(u, 1)
        finish(u, 2)

        @pl.when(u == last)
        def _():
            for part in range(pieces):
                for array in range(3):
                    x_copy(last, array, part_rows(part, pieces), x_last_sem(array, part)).start()

    row_step = 16

    def over_rows(part, parts, body):
        count = rows // parts
        if count == row_step:
            body(pl.ds(part * count, count))
            return

        def some_rows(i, carry):
            body(pl.ds(pl.multiple_of(part * count + i * row_step, row_step), row_step))
            return carry

        lax.fori_loop(0, count // row_step, some_rows, 0)

    def activate(u, part, parts, recv, slot):
        second, q, b = place(u)
        span = part_rows(part, parts)
        x_pair_arrival(u, span, recv).wait_recv()

        def body(lines):
            gate_sum = own_v[u, 0, lines, :] + f32(x_recv_v[u, 0, lines, :])
            up_sum = own_v[u, 1, lines, :] + f32(x_recv_v[u, 1, lines, :])
            sigmoid_gate = jax.nn.sigmoid(gate_sum)
            swish = gate_sum * sigmoid_gate
            hid_v[core, hid_slot(second), b, lines, :] = bf16(swish * up_sum)
            own_v[u, 0, lines, :] = up_sum * sigmoid_gate * (1.0 + gate_sum * (1.0 - sigmoid_gate))
            own_v[u, 1, lines, :] = swish

        over_rows(part, parts, body)
        nearh_copy(u, span, slot, core).start()

        @pl.when(second == 0)
        def _():
            yh_copy(b, span).start()

    def factors(u, part, parts, recv, slot):
        second, q, b = place(u)
        span = part_rows(part, parts)
        x_copy(u, 2, span, recv).wait_recv()

        def body(lines):
            hidden_grad = own_v[u, 2, lines, :] + f32(x_recv_v[u, 2, lines, :])
            grad_v[q, 0, 0, b, lines, core_lanes] = bf16(hidden_grad * own_v[u, 0, lines, :])
            grad_v[q, 1, 0, b, lines, core_lanes] = bf16(hidden_grad * own_v[u, 1, lines, :])

        over_rows(part, parts, body)
        y_copy(u, span, slot).start()
        near_copy(u, span).start()

    def elementwise(u):
        for half in range(halves):
            activate(u, half, halves, x_sem(u, 0, half), u)
            factors(u, half, halves, x_sem(u, 2, half), u)

    def mix_part(u):
        second, q, b = place(u)
        nearh_copy(u, pl.ds(0, rows), u, other).wait_recv()

        part = jnp.zeros((rows, feats), jnp.float32)
        for side in range(2):
            part = part + jnp.dot(
                hid_v[side, hid_slot(second), b], down_v[2 * q + side], preferred_element_type=jnp.float32
            )

        @pl.when(second == 0)
        def _():
            mix_acc_v[b] = part

        @pl.when((second == 1) & (b == 0))
        def _():
            mix_acc_v[0] = mix_acc_v[0] + part

        @pl.when((second == 1) & (b > 0))
        def _():
            mix_send_v[b] = bf16(mix_acc_v[b] + part)

        for static_b in range(2, blocks):

            @pl.when((second == 1) & (b == static_b))
            def _():
                mix_copy(static_b).start()

    def mix_last(half):
        second, q, b = place(last)
        span = part_rows(half, halves)
        part = mix_acc_v[b, span, :]
        for side in (core, other):
            if side is other:
                nearh_copy(last, span, last + half, other).wait_recv()
            part = part + jnp.dot(
                hid_v[side, 0, b, span, :], down_v[2 * q + side], preferred_element_type=jnp.float32
            )
        mix_send_v[b, span, :] = bf16(part)
        mix_last_copy(half).start()

    def spread_far():
        yt_copy(0).wait_recv()
        yt_copy(1).wait_recv()
        for b in range(1, blocks):
            zf_copy(0, b).start()
            zf_copy(1, b).start()

    def far_arrived(u):
        second, q, b = place(u)

        @pl.when(second == 0)
        def _():
            yh_arrival(b).wait_recv()
            fwdh_copy(b).start()

        whole = pl.ds(0, rows)
        y_arrival(u, whole, u).wait_recv()
        fwd_copy(u, whole).start()

    def last_far(part):
        span = part_rows(part, pieces)
        y_arrival(last, span, last + part).wait_recv()
        fwd_copy(last, span).start()

    def turn_tokens():
        all_arrived(tok_far.at[1:blocks], 0)
        all_arrived(cot_v.at[1, 1:blocks], 1)
        half_rows = blocks * rows
        own = tok_v[:, :, pl.ds(pl.multiple_of(layer * half_feats, 128), half_feats)]
        tok_turned[:, :half_rows] = own.reshape(half_rows, half_feats).T
        tok_turned[:, half_rows:] = tok_far[...].reshape(half_rows, half_feats).T

    def down_grad(side, half):
        if half == 0:
            hid_turned[...] = hid_v[side, 0:2].reshape(2 * blocks * rows, quarter).T
        lanes = slice(half * half_feats, (half + 1) * half_feats)
        down_grad_v[side, :, lanes] = bf16(
            jnp.dot(
                hid_turned[...],
                cot_v[:, :, :, lanes].reshape(2 * blocks * rows, half_feats),
                preferred_element_type=jnp.float32,
            )
        )

    stages = (
        (elementwise, 2, last),
        (compute_unit, 0, units),
        (mix_part, 2, last),
        (far_arrived, 3, last - 1),
    )

    def step(s, carry):
        for stage, lag, count in stages:

            @pl.when((s >= lag) & (s < count + lag))
            def _():
                stage(s - lag)

        pl.when(s == 4)(spread_far)
        pl.when(s == units)(turn_tokens)
        return carry

    lax.fori_loop(0, units + 1, step, 0)
    for part in range(pieces):
        half = part // 2
        activate(last, part, pieces, x_last_sem(0, part), last + half)
        factors(last, part, pieces, x_last_sem(2, part), last + part)
        if part == 1:
            mix_last(0)
    far_arrived(last - 1)
    down_grad(core, 0)
    last_far(0)
    mix_last(1)
    last_far(1)
    down_grad(core, 1)
    last_far(2)
    all_arrived(hid_v.at[other, 1], 4)
    down_grad(other, 0)
    last_far(3)
    down_grad(other, 1)

    total = mix_acc_v[0]
    for b in range(2, blocks):
        mix_copy(b).wait_recv()
        total = total + f32(mix_recv_v[b])
    for half in range(halves):
        mix_last_copy(half).wait_recv()
    total = total + f32(mix_recv_v[1])
    mix_v[...] = bf16(total)

    all_arrived(grad_v.at[:, :, 0, :, :, other_lanes], 2)
    all_arrived(grad_v.at[:, :, 1, :, :, other_lanes], 3)
    all_sent(core_send_v, 0)
    all_sent(tok_v.at[1:blocks], 1)
    all_sent(cot_v.at[0, 1:blocks], 2)
    all_sent(tok_far.at[0], 3)
    all_sent(cot_v.at[0, 0], 4)
    all_sent(tok_far.at[1:blocks], 5)
    all_sent(cot_v.at[1, 1:blocks], 6)
    all_sent(x_send_v, 7)
    all_sent(grad_v.at[:, :, 0, :, :, core_lanes], 8)
    all_sent(hid_v.at[core, 0:2], 9)
    all_sent(grad_v.at[:, :, 0, :, :, core_lanes], 10)
    all_sent(hid_v.at[core, 2], 11)
    all_sent(grad_v.at[:, :, 1, :, :, core_lanes], 12)
    all_sent(hid_v.at[core, 1], 13)
    all_sent(mix_send_v.at[1:blocks], 14)


def gradient_kernel(
    mix_v, tok_turned, down_grad_v, grad_v, mixed, grad_gate, grad_up, grad_down, wide_v, done, wide_sem
):
    half_hid = grad_v.shape[-1]
    quarter = half_hid // 2
    all_rows = tok_turned.shape[1]
    cut = min(half_hid, -(-half_hid // 512) * 256)
    mix_copy = pltpu.make_async_copy(mix_v, mixed, done.at[0])
    down_copies = [
        pltpu.make_async_copy(
            down_grad_v.at[side], grad_down.at[pl.ds(side * quarter, quarter)], done.at[1 + side]
        )
        for side in range(2)
    ]
    mix_copy.start()
    for copy in down_copies:
        copy.start()
    copies = []
    for q in range(2):
        for array in range(2):
            for start, stop in ((0, cut), (cut, half_hid)):
                slot = len(copies) % 4
                if len(copies) >= 4:
                    copies[-4].wait()
                factor = grad_v[q, array, :, :, :, start:stop].reshape(all_rows, stop - start)
                piece = wide_v.at[slot, :, 0 : stop - start]
                piece[...] = bf16(
                    jnp.dot(tok_turned[...], factor, preferred_element_type=jnp.float32)
                )
                target = (grad_gate, grad_up)[array]
                lanes = slice(q * half_hid + start, q * half_hid + stop)
                copies.append(pltpu.make_async_copy(piece, target.at[:, lanes], wide_sem.at[slot]))
                copies[-1].start()
    for copy in copies[-4:]:
        copy.wait()
    mix_copy.wait()
    for copy in down_copies:
        copy.wait()


def gradients(mixed, tok, down_grad, grad):
    half_feats, half_hid = tok.shape[0], grad.shape[-1]
    cut = min(half_hid, -(-half_hid // 512) * 256)
    narrow = jnp.bfloat16
    dma = pltpu.SemaphoreType.DMA
    return pl.pallas_call(
        gradient_kernel,
        out_shape=[
            jax.ShapeDtypeStruct(mixed.shape, narrow),
            jax.ShapeDtypeStruct((half_feats, 2 * half_hid), narrow),
            jax.ShapeDtypeStruct((half_feats, 2 * half_hid), narrow),
            jax.ShapeDtypeStruct((half_hid, down_grad.shape[2]), narrow),
        ],
        in_specs=[pl.BlockSpec(memory_space=pltpu.VMEM)] * 4,
        out_specs=[pl.BlockSpec(memory_space=pl.ANY)] * 4,
        scratch_shapes=[pltpu.VMEM((4, half_feats, cut), narrow), dma((3,)), dma((4,))],
        compiler_params=pltpu.CompilerParams(vmem_limit_bytes=VMEM_GRADS),
    )(mixed, tok, down_grad, grad)


def grid_device(n_row, n_col, tokens, w_gate, w_up, w_down, cotangent):
    rows, feats = tokens.shape
    hid = w_gate.shape[1]
    quarter = hid // 4
    blocks = n_col
    units = 2 * blocks
    all_rows = 2 * blocks * rows
    narrow, wide = jnp.bfloat16, jnp.float32
    dma = pltpu.SemaphoreType.DMA
    results = pl.pallas_call(
        functools.partial(exchange_kernel, n_row, n_col),
        out_shape=[
            pltpu.VMEM((rows, feats), narrow),
            pltpu.VMEM((feats // 2, all_rows), narrow),
            pltpu.VMEM((2, quarter, feats), narrow),
            pltpu.VMEM((2, 2, 2, blocks, rows, 2 * quarter), narrow),
        ],
        in_specs=[pl.BlockSpec(memory_space=pl.ANY)] * 5,
        out_specs=[pl.BlockSpec(memory_space=pltpu.VMEM)] * 4,
        scratch_shapes=[
            pltpu.VMEM((blocks, rows, feats), narrow),
            pltpu.VMEM((blocks, rows, feats // 2), narrow),
            pltpu.VMEM((2, blocks, rows, feats), narrow),
            pltpu.VMEM((2, 3, blocks, rows, quarter), narrow),
            pltpu.VMEM((quarter, all_rows), narrow),
            pltpu.VMEM((4, feats, quarter), narrow),
            pltpu.VMEM((4, feats, quarter), narrow),
            pltpu.VMEM((4, quarter, feats), narrow),
            pltpu.VMEM((units, 3, rows, quarter), narrow),
            pltpu.VMEM((units, 3, rows, quarter), narrow),
            pltpu.VMEM((units, 3, rows, quarter), wide),
            pltpu.VMEM((units, 3, rows, quarter), narrow),
            pltpu.VMEM((units, 3, rows, quarter), narrow),
            pltpu.VMEM((blocks, rows, feats), wide),
            pltpu.VMEM((blocks, rows, feats), narrow),
            pltpu.VMEM((blocks, rows, feats), narrow),
            dma((2,)),
            dma((7,)),
            dma((15,)),
            dma((5,)),
            dma((2, blocks)),
            dma((2,)),
            dma((units, 3)),
            dma((units - 1, 2, 2)),
            dma((2, 4)),
            dma((units + 1,)),
            dma((units + 3,)),
            dma((blocks,)),
            dma((blocks,)),
        ],
        compiler_params=pltpu.CompilerParams(
            collective_id=0, has_side_effects=True, vmem_limit_bytes=VMEM_LIMIT
        ),
    )(tokens, w_gate, w_up, w_down, cotangent)
    return tuple(gradients(*results))


def solution(mesh):
    placed = (
        P(("col", "depth"), "row"),
        P("row", "col"),
        P("row", "col"),
        P("col", "row"),
        P(("col", "depth"), "row"),
    )
    n_row, n_col = mesh.shape["row"], mesh.shape["col"]
    if (n_row, n_col, mesh.shape["depth"]) == (4, 4, 2):
        per_device = functools.partial(grid_device, n_row, n_col)
    else:
        per_device = layered_device
    return jax.shard_map(
        per_device,
        mesh=mesh,
        in_specs=placed,
        out_specs=(
            P(("col", "depth"), "row"),
            P(("row", "depth"), "col"),
            P(("row", "depth"), "col"),
            P(("col", "depth"), "row"),
        ),
        check_vma=False,
    )
```

```python
import functools

import jax
import jax.numpy as jnp
from jax import lax
from jax.experimental import pallas as pl
from jax.experimental.pallas import tpu as pltpu
from jax.sharding import PartitionSpec as P

COLS_CONTRACT = (((1,), (1,)), ((), ()))
ROWS_CONTRACT = (((0,), (0,)), ((), ()))


def gate_grads(hidden_grad, gate_sum, up_sum):
    sigmoid_gate = jax.nn.sigmoid(gate_sum)
    d_gate = (hidden_grad * up_sum * sigmoid_gate * (1.0 + gate_sum * (1.0 - sigmoid_gate))).astype(
        jnp.bfloat16
    )
    d_up = (hidden_grad * gate_sum * sigmoid_gate).astype(jnp.bfloat16)
    return (d_gate, d_up)


def layered_device(tokens, w_gate, w_up, w_down, cotangent):
    hid_width = w_gate.shape[1]
    token_rows = lax.all_gather(tokens, "col", axis=0, tiled=True)
    row_piece = token_rows
    joined = lax.psum_scatter(
        jnp.concatenate(
            [
                jnp.dot(row_piece, w_gate, preferred_element_type=jnp.float32),
                jnp.dot(row_piece, w_up, preferred_element_type=jnp.float32),
            ],
            axis=1,
        ).astype(jnp.bfloat16),
        "row",
        scatter_dimension=0,
        tiled=True,
    ).astype(jnp.float32)
    gate_sum = joined[:, :hid_width]
    up_sum = joined[:, hid_width:]
    hidden = (jax.nn.silu(gate_sum) * up_sum).astype(jnp.bfloat16)
    hidden_rows = lax.all_gather(hidden, "row", axis=0, tiled=True)
    row_piece = hidden_rows
    mixed = lax.psum_scatter(
        jnp.dot(row_piece, w_down, preferred_element_type=jnp.float32).astype(jnp.bfloat16),
        "col",
        scatter_dimension=0,
        tiled=True,
    )
    cot_rows = lax.all_gather(cotangent, "col", axis=0, tiled=True)
    row_piece = cot_rows
    hidden_grad = lax.psum_scatter(
        lax.dot_general(
            row_piece, w_down, COLS_CONTRACT, preferred_element_type=jnp.float32
        ).astype(jnp.bfloat16),
        "row",
        scatter_dimension=0,
        tiled=True,
    ).astype(jnp.float32)
    d_gate, d_up = gate_grads(hidden_grad, gate_sum, up_sum)
    d_gate_rows, d_up_rows = (
        lax.all_gather(d_gate, "row", axis=0, tiled=True),
        lax.all_gather(d_up, "row", axis=0, tiled=True),
    )
    down_term = lax.dot_general(
        hidden_rows, cot_rows, ROWS_CONTRACT, preferred_element_type=jnp.float32
    )
    grad_down = lax.psum_scatter(
        down_term.astype(jnp.bfloat16), "depth", scatter_dimension=0, tiled=True
    )
    layer_tokens = lax.all_to_all(token_rows, "depth", split_axis=1, concat_axis=0, tiled=True)
    block_rows = token_rows.shape[0]
    empty_grad = jnp.zeros((layer_tokens.shape[1], d_gate_rows.shape[1]), jnp.float32)
    first_row = jnp.int32(0)
    gate_total = empty_grad
    up_total = empty_grad
    gate_piece = lax.all_gather(d_gate_rows, "depth", axis=0, tiled=True)
    up_piece = lax.all_gather(d_up_rows, "depth", axis=0, tiled=True)
    for sub_index in range(gate_piece.shape[0] // block_rows):
        gate_block = gate_piece[sub_index * block_rows : (sub_index + 1) * block_rows]
        up_block = up_piece[sub_index * block_rows : (sub_index + 1) * block_rows]
        offset = first_row + sub_index * block_rows
        tok_block = lax.dynamic_slice_in_dim(layer_tokens, offset, block_rows, 0)
        gate_part = lax.optimization_barrier(
            lax.dot_general(
                tok_block, gate_block, ROWS_CONTRACT, preferred_element_type=jnp.float32
            ).astype(jnp.bfloat16)
        )
        up_part = lax.optimization_barrier(
            lax.dot_general(
                tok_block, up_block, ROWS_CONTRACT, preferred_element_type=jnp.float32
            ).astype(jnp.bfloat16)
        )
        gate_total = gate_total + gate_part.astype(jnp.float32)
        up_total = up_total + up_part.astype(jnp.float32)
    return (mixed, gate_total.astype(jnp.bfloat16), up_total.astype(jnp.bfloat16), grad_down)


MESH = pl.DeviceIdType.MESH
VMEM_LIMIT = 50_000_000
VMEM_GRADS = 32_000_000


def f32(x):
    return x.astype(jnp.float32)


def bf16(x):
    return x.astype(jnp.bfloat16)


def rows_dot(x, y):
    return lax.dot_general(x, y, ROWS_CONTRACT, preferred_element_type=jnp.float32)


def exchange_kernel(
    n_row,
    n_col,
    tok_in,
    gate_in,
    up_in,
    down_in,
    cot_in,
    mix_v,
    tok_turned,
    down_grad_v,
    grad_v,
    tok_v,
    tok_far,
    cot_v,
    hid_v,
    hid_turned,
    gate_v,
    up_v,
    down_v,
    core_send_v,
    core_recv_v,
    own_v,
    x_send_v,
    x_recv_v,
    mix_acc_v,
    mix_send_v,
    mix_recv_v,
    load_tok_sem,
    load_w_sem,
    sent,
    late,
    z_recv,
    yt_recv,
    core_recv,
    x_recv,
    x_last,
    nearh_recv,
    y_recv,
    yh_recv,
    mix_recv,
):
    row, col, layer = lax.axis_index("row"), lax.axis_index("col"), lax.axis_index("depth")
    core = row % 2
    other = 1 - core
    far_layer = 1 - layer
    blocks, rows, feats = tok_v.shape
    half_feats = tok_far.shape[2]
    quarter = gate_v.shape[2]
    units = x_send_v.shape[0]

    core_lanes = pl.ds(pl.multiple_of(core * quarter, 128), quarter)
    other_lanes = pl.ds(pl.multiple_of(other * quarter, 128), quarter)

    core_id = (row + 1 - 2 * core, col, layer)
    x_id = ((row + 2) % n_row, col, layer)
    y_id = (row, col, far_layer)
    z_ids = {
        1: (row, col + 1 - 2 * (col % 2), layer),
        2: (row, (col + 2) % n_col, layer),
        3: (row, n_col - 1 - col, layer),
    }

    def place(u):
        skip, final = (u + units - 3) // units, (u + 1) // units
        second = (u + skip) % 2 + final
        return second, (second + far_layer) % 2, (u + skip) // 2 - (blocks - 1) * final

    def remote(src, dst, send, recv, device):
        return pltpu.make_async_remote_copy(
            src_ref=src, dst_ref=dst, send_sem=send, recv_sem=recv, device_id=device, device_id_type=MESH
        )

    def weight_sem(array, second, own):
        if second == 0 and array == 0:
            return load_w_sem.at[own]
        return load_w_sem.at[1 + array + 3 * second]

    def load_weight(array, second):
        for own, side in ((0, other), (1, core)):
            part = 2 * ((second + far_layer) % 2) + side
            source = (gate_in, up_in, down_in)[array]
            target = (gate_v, up_v, down_v)[array]
            span = pl.ds(pl.multiple_of(part * quarter, 128), quarter)
            view = source.at[span, :] if array == 2 else source.at[:, span]
            pltpu.make_async_copy(view, target.at[part], weight_sem(array, second, own)).start()

    def weight_wait(array, second, own):
        source = (gate_in, up_in, down_in)[array]
        target = (gate_v, up_v, down_v)[array]
        single = second == 0 and array == 0
        wide = quarter if single else 2 * quarter
        view = source.at[0:wide, :] if array == 2 else source.at[:, 0:wide]
        pltpu.make_async_copy(view, view, weight_sem(array, second, own)).wait()

    load_tok = pltpu.make_async_copy(tok_in, tok_v.at[0], load_tok_sem.at[0])
    load_cot = pltpu.make_async_copy(cot_in, cot_v.at[0, 0], load_tok_sem.at[1])
    load_tok.start()
    load_cot.start()
    load_weight(0, 0)

    barrier = pltpu.get_barrier_semaphore()
    peers = [core_id, x_id, y_id] + [z_ids[b] for b in range(1, blocks)]
    for peer in peers:
        pl.semaphore_signal(barrier, inc=1, device_id=peer, device_id_type=MESH)

    def core_copy(u, a):
        return remote(
            core_send_v.at[u, a],
            core_recv_v.at[u, a],
            sent.at[0],
            core_recv.at[u, (a + 1) // 2],
            core_id,
        )

    def product(u, array, side):
        second, q, b = place(u)
        part = 2 * q + side
        if array == 2:
            return lax.dot_general(
                cot_v[0, b], down_v[part], COLS_CONTRACT, preferred_element_type=jnp.float32
            )
        weight = (gate_v, up_v)[array]
        return jnp.dot(tok_v[b], weight[part], preferred_element_type=jnp.float32)

    load_tok.wait()
    weight_wait(0, 0, 0)
    load_weight(1, 0)
    core_send_v[0, 0] = bf16(product(0, 0, other))
    pl.semaphore_wait(barrier, len(peers))
    core_copy(0, 0).start()

    def z_copy(array, b):
        buffer = (tok_v, cot_v.at[0])[array]
        return remote(buffer.at[0], buffer.at[b], sent.at[1 + array], z_recv.at[array, b], z_ids[b])

    z_copy(0, 1).start()
    load_cot.wait()
    z_copy(1, 1).start()
    for b in range(2, blocks):
        z_copy(0, b).start()
        z_copy(1, b).start()

    def yt_copy(array):
        if array == 0:
            lanes = pl.ds(pl.multiple_of(far_layer * half_feats, 128), half_feats)
            return remote(tok_v.at[0, :, lanes], tok_far.at[0], sent.at[3], yt_recv.at[0], y_id)
        return remote(cot_v.at[0, 0], cot_v.at[1, 0], sent.at[4], yt_recv.at[1], y_id)

    yt_copy(0).start()
    yt_copy(1).start()

    def zf_copy(array, b):
        buffer = (tok_far, cot_v.at[1])[array]
        return remote(buffer.at[0], buffer.at[b], sent.at[5 + array], late.at[array], z_ids[b])

    last = units - 1
    halves, pieces = 2, 4

    def part_rows(part, parts):
        return pl.ds(part * (rows // parts), rows // parts)

    def x_copy(u, a, span, recv):
        return remote(x_send_v.at[u, a, span], x_recv_v.at[u, a, span], sent.at[7], recv, x_id)

    def x_sem(u, a, part):
        return x_recv.at[u, part]

    def x_last_sem(a, part):
        return x_last.at[a // 2, part]

    def x_arrival(u, count, span, recv):
        ref = x_recv_v.at[u, 0:count, span]
        return remote(ref, ref, sent.at[7], recv, x_id)

    def near_copy(u, span):
        second, q, b = place(u)
        ref = grad_v.at[q, :, 0, b, span, core_lanes]
        return remote(ref, ref, sent.at[8], late.at[2], core_id)

    def hid_slot(second):
        return 2 - 2 * second

    def nearh_copy(u, span, slot, side):
        second, q, b = place(u)
        ref = hid_v.at[side, hid_slot(second), b, span]
        return remote(ref, ref, sent.at[9], nearh_recv.at[slot], core_id)

    def y_copy(u, span, slot):
        second, q, b = place(u)
        return remote(
            grad_v.at[q, :, 0, b, span, core_lanes],
            grad_v.at[q, :, 1, b, span, core_lanes],
            sent.at[8],
            y_recv.at[slot],
            y_id,
        )

    def y_arrival(u, span, slot):
        second, q, b = place(u)
        ref = grad_v.at[1 - q, :, 1, b, span, core_lanes]
        return remote(ref, ref, sent.at[8], y_recv.at[slot], y_id)

    def yh_copy(b, span):
        return remote(
            hid_v.at[core, 2, b, span], hid_v.at[core, 1, b, span], sent.at[11], yh_recv.at[b], y_id
        )

    def yh_arrival(b):
        ref = hid_v.at[core, 1, b]
        return remote(ref, ref, sent.at[11], yh_recv.at[b], y_id)

    def fwd_copy(u, span):
        second, q, b = place(u)
        ref = grad_v.at[1 - q, :, 1, b, span, core_lanes]
        return remote(ref, ref, sent.at[12], late.at[3], core_id)

    def fwdh_copy(b):
        ref = hid_v.at[core, 1, b]
        return remote(ref, ref, sent.at[13], late.at[4], core_id)

    def mix_copy(b):
        return remote(mix_send_v.at[b], mix_recv_v.at[b], sent.at[10], mix_recv.at[b], z_ids[b])

    def mix_last_copy(half):
        span = part_rows(half, halves)
        return remote(
            mix_send_v.at[1, span], mix_recv_v.at[1, span], sent.at[10], mix_recv.at[half], z_ids[1]
        )

    def all_sent(ref, slot):
        remote(ref, ref, sent.at[slot], late.at[0], core_id).wait_send()

    def all_arrived(ref, slot):
        remote(ref, ref, sent.at[0], late.at[slot], core_id).wait_recv()

    def products(u, array):
        def for_other():
            core_send_v[u, array] = bf16(product(u, array, other))
            core_copy(u, array).start()

        if array == 0:
            pl.when(u > 0)(for_other)
        else:
            for_other()
        own_v[u, array] = product(u, array, core)

    def finish(u, array):
        if array == 0:
            core_copy(u, 0).wait_recv()
        elif array == 1:
            ref = core_recv_v.at[u, 1:3]
            remote(ref, ref, sent.at[0], core_recv.at[u, 1], core_id).wait_recv()
        total = own_v[u, array] + f32(core_recv_v[u, array])
        own_v[u, array] = total
        x_send_v[u, array] = bf16(total)

        @pl.when(u < last)
        def _():
            for half in range(halves):
                x_copy(u, array, part_rows(half, halves), x_sem(u, array, half)).start()

    def wait_weight(u, array):
        for second in range(2):

            @pl.when(u == second)
            def _():
                weight_wait(array, second, 1)

    def compute_unit(u):
        second, q, b = place(u)

        for static_b in range(1, blocks):

            @pl.when((b == static_b) & (second == 0))
            def _():
                z_copy(0, static_b).wait_recv()

        wait_weight(u, 0)

        @pl.when(u == 0)
        def _():
            load_weight(2, 0)

        products(u, 0)

        @pl.when(u == 0)
        def _():
            finish(u, 0)

        wait_weight(u, 1)

        @pl.when(u == 0)
        def _():
            for array in range(3):
                load_weight(array, 1)

        products(u, 1)

        @pl.when(u > 0)
        def _():
            finish(u, 0)

        for static_b in range(1, blocks):

            @pl.when((b == static_b) & (second == 0))
            def _():
                z_copy(1, static_b).wait_recv()

        wait_weight(u, 2)
        products(u, 2)
        finish(u, 1)
        finish(u, 2)

        @pl.when(u == last)
        def _():
            for part in range(pieces):
                for array in range(3):
                    x_copy(last, array, part_rows(part, pieces), x_last_sem(array, part)).start()

    row_step = 16

    def over_rows(part, parts, body):
        count = rows // parts
        if count == row_step:
            body(pl.ds(part * count, count))
            return

        def some_rows(i, carry):
            body(pl.ds(pl.multiple_of(part * count + i * row_step, row_step), row_step))
            return carry

        lax.fori_loop(0, count // row_step, some_rows, 0)

    def activate(u, part, parts, recv, slot):
        second, q, b = place(u)
        span = part_rows(part, parts)
        x_arrival(u, 2 if parts == pieces else 3, span, recv).wait_recv()

        def body(lines):
            gate_sum = own_v[u, 0, lines, :] + f32(x_recv_v[u, 0, lines, :])
            up_sum = own_v[u, 1, lines, :] + f32(x_recv_v[u, 1, lines, :])
            sigmoid_gate = jax.nn.sigmoid(gate_sum)
            swish = gate_sum * sigmoid_gate
            hid_v[core, hid_slot(second), b, lines, :] = bf16(swish * up_sum)
            own_v[u, 0, lines, :] = up_sum * sigmoid_gate * (1.0 + gate_sum * (1.0 - sigmoid_gate))
            own_v[u, 1, lines, :] = swish

        over_rows(part, parts, body)
        nearh_copy(u, span, slot, core).start()

        @pl.when(second == 0)
        def _():
            yh_copy(b, span).start()

    def factors(u, part, parts, recv, slot):
        second, q, b = place(u)
        span = part_rows(part, parts)
        if parts == pieces:
            x_copy(u, 2, span, recv).wait_recv()

        def body(lines):
            hidden_grad = own_v[u, 2, lines, :] + f32(x_recv_v[u, 2, lines, :])
            grad_v[q, 0, 0, b, lines, core_lanes] = bf16(hidden_grad * own_v[u, 0, lines, :])
            grad_v[q, 1, 0, b, lines, core_lanes] = bf16(hidden_grad * own_v[u, 1, lines, :])

        over_rows(part, parts, body)
        y_copy(u, span, slot).start()
        near_copy(u, span).start()

    def elementwise(u):
        for half in range(halves):
            activate(u, half, halves, x_sem(u, 0, half), u)
            factors(u, half, halves, x_sem(u, 2, half), u)

    def mix_part(u):
        second, q, b = place(u)
        nearh_copy(u, pl.ds(0, rows), u, other).wait_recv()

        part = jnp.zeros((rows, feats), jnp.float32)
        for side in range(2):
            part = part + jnp.dot(
                hid_v[side, hid_slot(second), b], down_v[2 * q + side], preferred_element_type=jnp.float32
            )

        @pl.when(second == 0)
        def _():
            mix_acc_v[b] = part

        @pl.when((second == 1) & (b == 0))
        def _():
            mix_acc_v[0] = mix_acc_v[0] + part

        @pl.when((second == 1) & (b > 0))
        def _():
            mix_send_v[b] = bf16(mix_acc_v[b] + part)

        for static_b in range(2, blocks):

            @pl.when((second == 1) & (b == static_b))
            def _():
                mix_copy(static_b).start()

    def mix_last(half):
        second, q, b = place(last)
        span = part_rows(half, halves)
        part = mix_acc_v[b, span, :]
        for side in (core, other):
            if side is other:
                nearh_copy(last, span, last + half, other).wait_recv()
            part = part + jnp.dot(
                hid_v[side, 0, b, span, :], down_v[2 * q + side], preferred_element_type=jnp.float32
            )
        mix_send_v[b, span, :] = bf16(part)
        mix_last_copy(half).start()

    def spread_far():
        yt_copy(0).wait_recv()
        yt_copy(1).wait_recv()
        for b in range(1, blocks):
            zf_copy(0, b).start()
            zf_copy(1, b).start()

    def far_arrived(u):
        second, q, b = place(u)

        @pl.when(second == 0)
        def _():
            yh_arrival(b).wait_recv()
            fwdh_copy(b).start()

        whole = pl.ds(0, rows)
        y_arrival(u, whole, u).wait_recv()
        fwd_copy(u, whole).start()

    def last_far(part):
        span = part_rows(part, pieces)
        y_arrival(last, span, last + part).wait_recv()
        fwd_copy(last, span).start()

    def turn_tokens():
        all_arrived(tok_far.at[1:blocks], 0)
        all_arrived(cot_v.at[1, 1:blocks], 1)
        half_rows = blocks * rows
        own = tok_v[:, :, pl.ds(pl.multiple_of(layer * half_feats, 128), half_feats)]
        tok_turned[:, :half_rows] = own.reshape(half_rows, half_feats).T
        tok_turned[:, half_rows:] = tok_far[...].reshape(half_rows, half_feats).T

    def down_grad(side, half):
        if half == 0:
            hid_turned[...] = hid_v[side, 0:2].reshape(2 * blocks * rows, quarter).T
        lanes = slice(half * half_feats, (half + 1) * half_feats)
        down_grad_v[side, :, lanes] = bf16(
            jnp.dot(
                hid_turned[...],
                cot_v[:, :, :, lanes].reshape(2 * blocks * rows, half_feats),
                preferred_element_type=jnp.float32,
            )
        )

    stages = (
        (elementwise, 2, last),
        (compute_unit, 0, units),
        (mix_part, 2, last),
        (far_arrived, 3, last - 1),
    )

    def step(s, carry):
        for stage, lag, count in stages:

            @pl.when((s >= lag) & (s < count + lag))
            def _():
                stage(s - lag)

        pl.when(s == 4)(spread_far)
        pl.when(s == units)(turn_tokens)
        return carry

    lax.fori_loop(0, units + 1, step, 0)
    for part in range(pieces):
        half = part // 2
        activate(last, part, pieces, x_last_sem(0, part), last + half)
        factors(last, part, pieces, x_last_sem(2, part), last + part)
        if part == 1:
            mix_last(0)
    far_arrived(last - 1)
    down_grad(core, 0)
    last_far(0)
    mix_last(1)
    last_far(1)
    down_grad(core, 1)
    last_far(2)
    all_arrived(hid_v.at[other, 1], 4)
    down_grad(other, 0)
    last_far(3)
    down_grad(other, 1)

    total = mix_acc_v[0]
    for b in range(2, blocks):
        mix_copy(b).wait_recv()
        total = total + f32(mix_recv_v[b])
    for half in range(halves):
        mix_last_copy(half).wait_recv()
    total = total + f32(mix_recv_v[1])
    mix_v[...] = bf16(total)

    all_arrived(grad_v.at[:, :, 0, :, :, other_lanes], 2)
    all_arrived(grad_v.at[:, :, 1, :, :, other_lanes], 3)
    all_sent(core_send_v, 0)
    all_sent(tok_v.at[1:blocks], 1)
    all_sent(cot_v.at[0, 1:blocks], 2)
    all_sent(tok_far.at[0], 3)
    all_sent(cot_v.at[0, 0], 4)
    all_sent(tok_far.at[1:blocks], 5)
    all_sent(cot_v.at[1, 1:blocks], 6)
    all_sent(x_send_v, 7)
    all_sent(grad_v.at[:, :, :, :, :, core_lanes], 8)
    all_sent(hid_v.at[core, 0:2], 9)
    all_sent(hid_v.at[core, 2], 11)
    all_sent(grad_v.at[:, :, 1, :, :, core_lanes], 12)
    all_sent(hid_v.at[core, 1], 13)
    all_sent(mix_send_v.at[1:blocks], 10)


def gradient_kernel(
    mix_v, tok_turned, down_grad_v, grad_v, mixed, grad_gate, grad_up, grad_down, wide_v, done, wide_sem
):
    half_hid = grad_v.shape[-1]
    quarter = half_hid // 2
    all_rows = tok_turned.shape[1]
    cut = min(half_hid, -(-half_hid // 512) * 256)
    mix_copy = pltpu.make_async_copy(mix_v, mixed, done.at[0])
    down_copies = [
        pltpu.make_async_copy(
            down_grad_v.at[side], grad_down.at[pl.ds(side * quarter, quarter)], done.at[1 + side]
        )
        for side in range(2)
    ]
    mix_copy.start()
    for copy in down_copies:
        copy.start()
    copies = []
    for q in range(2):
        for array in range(2):
            for start, stop in ((0, cut), (cut, half_hid)):
                slot = len(copies) % 4
                if len(copies) >= 4:
                    copies[-4].wait()
                factor = grad_v[q, array, :, :, :, start:stop].reshape(all_rows, stop - start)
                piece = wide_v.at[slot, :, 0 : stop - start]
                piece[...] = bf16(
                    jnp.dot(tok_turned[...], factor, preferred_element_type=jnp.float32)
                )
                target = (grad_gate, grad_up)[array]
                lanes = slice(q * half_hid + start, q * half_hid + stop)
                copies.append(pltpu.make_async_copy(piece, target.at[:, lanes], wide_sem.at[slot]))
                copies[-1].start()
    for copy in copies[-4:]:
        copy.wait()
    mix_copy.wait()
    for copy in down_copies:
        copy.wait()


def gradients(mixed, tok, down_grad, grad):
    half_feats, half_hid = tok.shape[0], grad.shape[-1]
    cut = min(half_hid, -(-half_hid // 512) * 256)
    narrow = jnp.bfloat16
    dma = pltpu.SemaphoreType.DMA
    return pl.pallas_call(
        gradient_kernel,
        out_shape=[
            jax.ShapeDtypeStruct(mixed.shape, narrow),
            jax.ShapeDtypeStruct((half_feats, 2 * half_hid), narrow),
            jax.ShapeDtypeStruct((half_feats, 2 * half_hid), narrow),
            jax.ShapeDtypeStruct((half_hid, down_grad.shape[2]), narrow),
        ],
        in_specs=[pl.BlockSpec(memory_space=pltpu.VMEM)] * 4,
        out_specs=[pl.BlockSpec(memory_space=pl.ANY)] * 4,
        scratch_shapes=[pltpu.VMEM((4, half_feats, cut), narrow), dma((3,)), dma((4,))],
        compiler_params=pltpu.CompilerParams(vmem_limit_bytes=VMEM_GRADS),
    )(mixed, tok, down_grad, grad)


def grid_device(n_row, n_col, tokens, w_gate, w_up, w_down, cotangent):
    rows, feats = tokens.shape
    hid = w_gate.shape[1]
    quarter = hid // 4
    blocks = n_col
    units = 2 * blocks
    all_rows = 2 * blocks * rows
    narrow, wide = jnp.bfloat16, jnp.float32
    dma = pltpu.SemaphoreType.DMA
    results = pl.pallas_call(
        functools.partial(exchange_kernel, n_row, n_col),
        out_shape=[
            pltpu.VMEM((rows, feats), narrow),
            pltpu.VMEM((feats // 2, all_rows), narrow),
            pltpu.VMEM((2, quarter, feats), narrow),
            pltpu.VMEM((2, 2, 2, blocks, rows, 2 * quarter), narrow),
        ],
        in_specs=[pl.BlockSpec(memory_space=pl.ANY)] * 5,
        out_specs=[pl.BlockSpec(memory_space=pltpu.VMEM)] * 4,
        scratch_shapes=[
            pltpu.VMEM((blocks, rows, feats), narrow),
            pltpu.VMEM((blocks, rows, feats // 2), narrow),
            pltpu.VMEM((2, blocks, rows, feats), narrow),
            pltpu.VMEM((2, 3, blocks, rows, quarter), narrow),
            pltpu.VMEM((quarter, all_rows), narrow),
            pltpu.VMEM((4, feats, quarter), narrow),
            pltpu.VMEM((4, feats, quarter), narrow),
            pltpu.VMEM((4, quarter, feats), narrow),
            pltpu.VMEM((units, 3, rows, quarter), narrow),
            pltpu.VMEM((units, 3, rows, quarter), narrow),
            pltpu.VMEM((units, 3, rows, quarter), wide),
            pltpu.VMEM((units, 3, rows, quarter), narrow),
            pltpu.VMEM((units, 3, rows, quarter), narrow),
            pltpu.VMEM((blocks, rows, feats), wide),
            pltpu.VMEM((blocks, rows, feats), narrow),
            pltpu.VMEM((blocks, rows, feats), narrow),
            dma((2,)),
            dma((7,)),
            dma((14,)),
            dma((5,)),
            dma((2, blocks)),
            dma((2,)),
            dma((units, 2)),
            dma((units - 1, 2)),
            dma((2, 4)),
            dma((units + 1,)),
            dma((units + 3,)),
            dma((blocks,)),
            dma((blocks,)),
        ],
        compiler_params=pltpu.CompilerParams(
            collective_id=0, has_side_effects=True, vmem_limit_bytes=VMEM_LIMIT
        ),
    )(tokens, w_gate, w_up, w_down, cotangent)
    return tuple(gradients(*results))


def solution(mesh):
    placed = (
        P(("col", "depth"), "row"),
        P("row", "col"),
        P("row", "col"),
        P("col", "row"),
        P(("col", "depth"), "row"),
    )
    n_row, n_col = mesh.shape["row"], mesh.shape["col"]
    if (n_row, n_col, mesh.shape["depth"]) == (4, 4, 2):
        per_device = functools.partial(grid_device, n_row, n_col)
    else:
        per_device = layered_device
    return jax.shard_map(
        per_device,
        mesh=mesh,
        in_specs=placed,
        out_specs=(
            P(("col", "depth"), "row"),
            P(("row", "depth"), "col"),
            P(("row", "depth"), "col"),
            P(("col", "depth"), "row"),
        ),
        check_vma=False,
    )
```
